32 devices in a mesh: dp: 1 (over z), ep: 4 (over y), tp: 8 (over x, core).
Axes of the slice: x: 4, y: 4, z: 1, core: 2. Of those that a mesh axis runs over, the one named last changes fastest.
The devices are a block of a 4x4x8 slice.
Arguments:
- x_in: bfloat16 [4096, 2048], P(('dp', 'ep'))
- expert_ids: int32 [4096, 2], P(('dp', 'ep'))
- gate_vals: float32 [4096, 2], P(('dp', 'ep'))
- w_gate: bfloat16 [8, 2048, 7168], P('ep', None, 'tp')
- w_up: bfloat16 [8, 2048, 7168], P('ep', None, 'tp')
- w_down: bfloat16 [8, 7168, 2048], P('ep', 'tp')
Outputs:
- output: bfloat16 [4096, 2048], P(('dp', 'ep'))
All inputs are finite; a program needn't handle non-finite values.
Results may differ from the reference program's by a relative error of at most 0.00932271.
Values are sent between devices in bfloat16 or wider.
A program may use at most 768 MiB of HBM per device.

```python
import jax
import jax.numpy as jnp
from jax import lax

D = 2048
FF = 7168
EXPERTS = 8
TOP = 2
TOKENS = 1024
SOURCES = 4

CAPACITY = (5 * TOP * TOKENS) // (4 * EXPERTS)


def draw_routing(key, num_rows):
    scores = jax.random.randint(key, (num_rows, EXPERTS), 0, 1048576, dtype=jnp.int32)
    scores = scores * EXPERTS + jnp.arange(EXPERTS, dtype=jnp.int32)[None, :]
    _, chosen = lax.top_k(scores, TOP)
    return chosen.astype(jnp.int32)


def setup_inputs(seed: int = 0, part: int = 0) -> dict:
    base = jax.random.key(seed)
    key_x, key_ids, key_gate = jax.random.split(jax.random.fold_in(base, part), 3)
    key_wg, key_wu, key_wd = jax.random.split(jax.random.key(seed + 1), 3)
    num_rows = SOURCES * TOKENS
    x_in = jax.random.normal(key_x, (num_rows, D), jnp.float32).astype(jnp.bfloat16)
    expert_ids = draw_routing(key_ids, num_rows)
    gate_vals = jax.random.uniform(key_gate, (num_rows, TOP), jnp.float32, 0.25, 1.25)
    w_gate = (jax.random.normal(key_wg, (EXPERTS, D, FF), jnp.float32) * D ** -0.5).astype(jnp.bfloat16)
    w_up = (jax.random.normal(key_wu, (EXPERTS, D, FF), jnp.float32) * D ** -0.5).astype(jnp.bfloat16)
    w_down = (jax.random.normal(key_wd, (EXPERTS, FF, D), jnp.float32) * FF ** -0.5).astype(jnp.bfloat16)
    return {'x_in': x_in, 'expert_ids': expert_ids, 'gate_vals': gate_vals,
            'w_gate': w_gate, 'w_up': w_up, 'w_down': w_down}


def slot_numbers(ids_one):
    flat_ids = ids_one.reshape(TOKENS * TOP)
    onehot = (flat_ids[:, None] == jnp.arange(EXPERTS, dtype=jnp.int32)[None, :]).astype(jnp.int32)
    slots = jnp.sum((jnp.cumsum(onehot, axis=0) - onehot) * onehot, axis=1)
    return slots.reshape(TOKENS, TOP)


def reference(x_in, expert_ids, gate_vals, w_gate, w_up, w_down):
    x_src = x_in.reshape(SOURCES, TOKENS, D)
    ids_src = expert_ids.reshape(SOURCES, TOKENS, TOP)
    gates_src = gate_vals.reshape(SOURCES, TOKENS, TOP)
    slots = lax.map(slot_numbers, ids_src)
    kept = slots < CAPACITY
    flat_slot = jnp.where(kept, ids_src * CAPACITY + slots, EXPERTS * CAPACITY)
    token_num = jnp.broadcast_to(jnp.arange(TOKENS, dtype=jnp.int32)[:, None], (TOKENS, TOP))

    def dispatch(operands):
        tok_rows, slot_one = operands
        slot_owner = jnp.full((EXPERTS * CAPACITY + 1,), TOKENS, jnp.int32)
        slot_owner = slot_owner.at[slot_one.reshape(TOKENS * TOP)].set(token_num.reshape(TOKENS * TOP))
        padded = jnp.concatenate([tok_rows, jnp.zeros((1, D), tok_rows.dtype)], axis=0)
        return padded[slot_owner[: EXPERTS * CAPACITY]]

    slot_rows = lax.map(dispatch, (x_src, flat_slot))
    by_expert = slot_rows.reshape(SOURCES, EXPERTS, CAPACITY, D).transpose(1, 0, 2, 3)
    by_expert = by_expert.reshape(EXPERTS, SOURCES * CAPACITY, D)

    def expert_ffn(operands):
        rows_e, wg_e, wu_e, wd_e = operands
        gated = jax.nn.silu(jnp.dot(rows_e, wg_e, preferred_element_type=jnp.float32)) * jnp.dot(rows_e, wu_e, preferred_element_type=jnp.float32)
        hidden = gated.astype(jnp.bfloat16)
        return jnp.dot(hidden, wd_e, preferred_element_type=jnp.float32).astype(jnp.bfloat16)

    y_rows = lax.map(expert_ffn, (by_expert, w_gate, w_up, w_down))
    y_src = y_rows.reshape(EXPERTS, SOURCES, CAPACITY, D).transpose(1, 0, 2, 3)
    y_src = y_src.reshape(SOURCES, EXPERTS * CAPACITY, D)

    def combine(operands):
        y_one, slot_one, gate_one, kept_one = operands
        safe_slot = jnp.minimum(slot_one, EXPERTS * CAPACITY - 1)
        weight = jnp.where(kept_one, gate_one, 0.0)
        total = jnp.zeros((TOKENS, D), jnp.float32)
        for choice in range(TOP):
            total = total + weight[:, choice:choice + 1] * y_one[safe_slot[:, choice]].astype(jnp.float32)
        return total.astype(jnp.bfloat16)

    y_out = lax.map(combine, (y_src, flat_slot, gates_src, kept))
    return y_out.reshape(SOURCES * TOKENS, D)
```

```python
import jax
import jax.numpy as jnp
from jax import lax
from jax.experimental import pallas as pl
from jax.experimental.pallas import tpu as pltpu
from jax.sharding import PartitionSpec as P

CAP_NUM = 5
CAP_DEN = 4
LANES = 128
MESH = pl.DeviceIdType.MESH
BF16 = jnp.bfloat16
F32 = jnp.float32


def moe_kernel(n_ep, n_tp, cap,
               ids_ref, gates_ref, x_hbm, wg_hbm, wu_hbm, wd_hbm, out_hbm,
               xv, onehot, xs, xr, w1, wd, hid, part, rv, red, ret, acc, slots, cols, colsT, yb, agb,
               x_sem, w_sem, w_send, d_send, d_recv, rs_send, rs_recv, rt_send, rt_recv,
               ag_send, ag_recv, p_send, p_recv, o_sem):
    tokens, d_model = x_hbm.shape
    n_x = n_tp // 2
    n_tile = w1.shape[1]
    half_ff = wd.shape[1]
    n_col = part.shape[3]
    half_cap = cap // 2
    half_col = n_col // 2
    ep = lax.axis_index('ep')
    tp = lax.axis_index('tp')
    core = lax.rem(tp, 2)
    xpos = tp // 2
    partner = tp + 1 - 2 * core
    yp, y2, ym = [lax.rem(ep + i, n_ep) for i in (1, 2, 3)]

    def remote(src, dst, ss, rs, ep_to, tp_to):
        return pltpu.make_async_remote_copy(src_ref=src, dst_ref=dst, send_sem=ss, recv_sem=rs,
                                            device_id={'ep': ep_to, 'tp': tp_to}, device_id_type=MESH)

    x_copy = pltpu.make_async_copy(x_hbm, xv, x_sem.at[0])
    x_copy.start()

    def lanes(i):
        return pl.ds(i * LANES, LANES)

    for i in range(n_tile):
        pltpu.make_async_copy(wg_hbm.at[core, :, lanes(i)], w1.at[0, i, :, pl.ds(0, LANES)], w_sem.at[0]).start()
        pltpu.make_async_copy(wu_hbm.at[core, :, lanes(i)], w1.at[0, i, :, pl.ds(LANES, LANES)], w_sem.at[0]).start()
    pltpu.make_async_copy(wd_hbm.at[core], wd.at[0], w_sem.at[1]).start()

    barrier = pltpu.get_barrier_semaphore()
    peers = [(ep, partner)] + [(e, t) for e in (yp, ym, y2) for t in (tp, partner)]
    peers += [(ep, lax.rem(tp + 2 * d, n_tp)) for d in range(1, n_x)]
    for e, t in peers:
        pl.semaphore_signal(barrier, inc=1, device_id={'ep': e, 'tp': t}, device_id_type=MESH)

    n_row = slots.shape[0]
    expert = lax.broadcasted_iota(jnp.int32, (n_row, LANES), 0)
    low = lax.broadcasted_iota(jnp.int32, (LANES, LANES), 0)
    high = lax.broadcasted_iota(jnp.int32, (LANES, LANES), 1)
    before = jnp.where(low < high, 1.0, 0.0).astype(BF16)
    ones = jnp.ones((LANES, LANES), BF16)
    delta = lax.rem(expert // 2 - ep + n_ep, n_ep)
    piece = jnp.where(delta == 3, 1, jnp.where(delta == 1, 2, jnp.where(delta == 2, 3, 0)))
    base = ((piece * 2 + lax.rem(expert, 2)) * cap).astype(F32)
    carry = jnp.zeros((n_row, LANES), F32)
    cols[...] = jnp.zeros_like(cols)
    for b in range(tokens // LANES):
        hit = [expert == ids_ref[j:j + 1, b * LANES:(b + 1) * LANES] for j in range(2)]
        mask = jnp.where(hit[0] | hit[1], 1.0, 0.0)
        rank = jnp.dot(mask.astype(BF16), before, preferred_element_type=F32) + carry
        carry = carry + jnp.dot(mask.astype(BF16), ones, preferred_element_type=F32)
        kept = rank < float(cap)
        slots[:, b * LANES:(b + 1) * LANES] = jnp.where((mask > 0.0) & kept, rank, -1.0)
        where_to = jnp.where(kept, base + rank + 1.0, 0.0)
        for j in range(2):
            flat = jnp.sum(jnp.where(hit[j], where_to, 0.0), axis=0, keepdims=True) - 1.0
            cols[j:j + 1, b * LANES:(b + 1) * LANES] = flat
            cols[2 + j:3 + j, b * LANES:(b + 1) * LANES] = gates_ref[j:j + 1, b * LANES:(b + 1) * LANES]

    pl.semaphore_wait(barrier, len(peers))

    other = 1 - core
    for i in range(n_tile):
        remote(wg_hbm.at[other, :, lanes(i)], w1.at[1, i, :, pl.ds(0, LANES)], w_send.at[0], w_sem.at[2], ep, partner).start()
        remote(wu_hbm.at[other, :, lanes(i)], w1.at[1, i, :, pl.ds(LANES, LANES)], w_send.at[0], w_sem.at[2], ep, partner).start()
    remote(wd_hbm.at[other], wd.at[1], w_send.at[1], w_sem.at[3], ep, partner).start()

    x_copy.wait()

    def pick(expert_id, dst):
        row = slots[pl.ds(expert_id, 1), :]
        slot = lax.broadcasted_iota(jnp.int32, (cap, tokens), 0).astype(F32)
        onehot[...] = jnp.where(slot == row, 1.0, 0.0).astype(BF16)
        step = 512
        for c in range(d_model // step):
            dst[:, c * step:(c + 1) * step] = jnp.dot(
                onehot[...], xv[:, c * step:(c + 1) * step], preferred_element_type=F32).astype(BF16)

    top, bottom = pl.ds(0, half_cap), pl.ds(half_cap, half_cap)
    sends = [
        remote(xs.at[0, top], xr.at[1, bottom], d_send.at[0], d_recv.at[1], yp, tp),
        remote(xs.at[0, bottom], xr.at[2, bottom], d_send.at[1], d_recv.at[3], yp, tp),
        remote(xs.at[1, top], xr.at[1, top], d_send.at[2], d_recv.at[0], ym, tp),
        remote(xs.at[1, bottom], xr.at[2, top], d_send.at[3], d_recv.at[2], ym, tp),
        remote(xs.at[2], xr.at[3], d_send.at[4], d_recv.at[4], y2, tp),
    ]
    pick(2 * yp + core, xs.at[0])
    sends[0].start()
    sends[1].start()
    pick(2 * ym + core, xs.at[1])
    sends[2].start()
    sends[3].start()
    pick(2 * ep + core, xr.at[0])

    def here(ref, sem):
        pltpu.make_async_copy(ref, ref, sem).wait()

    def scatter(r, d):
        c = lax.rem(xpos + d, n_x)
        return remote(part.at[r, c], rv.at[r, d - 1], rs_send.at[r, d - 1], rs_recv.at[r, d - 1], ep, 2 * c + core)

    def returns(r):
        out = []
        for k in range(2):
            t = 2 * xpos + k
            if r == 3:
                out.append(remote(red.at[3, k], ret.at[3, core], rt_send.at[3, k, 0], rt_recv.at[3, core, 0], y2, t))
            else:
                to = pl.ds((r - 1) * half_cap, half_cap)
                out.append(remote(red.at[r, k, top], ret.at[1, core, to], rt_send.at[r, k, 0],
                                  rt_recv.at[1, core, r - 1], yp, t))
                out.append(remote(red.at[r, k, bottom], ret.at[2, core, to], rt_send.at[r, k, 1],
                                  rt_recv.at[2, core, r - 1], ym, t))
        return out

    def return_own():
        return remote(red.at[0, other], ret.at[0, core], rt_send.at[0, 0, 0], rt_recv.at[0, core, 0], ep, partner)

    def finish(r):
        for d in range(1, n_x):
            scatter(r, d).wait_recv()
        total = part[r, xpos].astype(F32)
        for d in range(1, n_x):
            total = total + rv[r, d - 1].astype(F32)
        total = total.astype(BF16)
        red[r, 0] = total[:, :half_col]
        red[r, 1] = total[:, half_col:]

    def chunk(r, _):
        @pl.when(r == 1)
        def _():
            here(xr.at[1, top], d_recv.at[0])
            here(xr.at[1, bottom], d_recv.at[1])

        @pl.when(r == 2)
        def _():
            here(xr.at[2, top], d_recv.at[2])
            here(xr.at[2, bottom], d_recv.at[3])

        @pl.when(r == 3)
        def _():
            here(xr.at[3], d_recv.at[4])

        def gate_up(h, _):
            @pl.when(r == 0)
            def _():
                here(w1.at[h], w_sem.at[2 * h])

            for i in range(n_tile):
                ab = jnp.dot(xr[r], w1[h, i], preferred_element_type=F32)
                a, b = ab[:, :LANES], ab[:, LANES:]
                hid[h, :, i * LANES:(i + 1) * LANES] = (jax.nn.silu(a) * b).astype(BF16)
            return 0

        lax.fori_loop(0, 2, gate_up, 0)

        @pl.when(r == 0)
        def _():
            here(wd.at[0], w_sem.at[1])
            here(wd.at[1], w_sem.at[3])

        def down(c, _):
            step = 256
            for i in range(n_col // step):
                span = pl.ds(pl.multiple_of(c * n_col + i * step, step), step)
                o = jnp.dot(hid[0], wd[0, :, span], preferred_element_type=F32)
                o = o + jnp.dot(hid[1], wd[1, :, span], preferred_element_type=F32)
                part[r, c, :, i * step:(i + 1) * step] = o.astype(BF16)
            return 0

        lax.fori_loop(0, n_x, down, 0)
        for d in range(1, n_x):
            scatter(r, d).start()

        @pl.when(r == 0)
        def _():
            pick(2 * y2 + core, xs.at[2])
            sends[4].start()
            for b in range(tokens // LANES):
                colsT[b * LANES:(b + 1) * LANES, :] = cols[:, b * LANES:(b + 1) * LANES].T

        @pl.when(r > 0)
        def _():
            finish(r - 1)

        @pl.when(r == 1)
        def _():
            return_own().start()
            ret[0, core] = red[0, core]

        for q in (1, 2):
            @pl.when(r == q + 1)
            def _():
                for copy in returns(q):
                    copy.start()
        return 0

    lax.fori_loop(0, 4, chunk, 0)

    acc[...] = jnp.zeros_like(acc)

    def combine(q):
        rows = tokens // 4

        def block(b, _):
            at = pl.ds(pl.multiple_of(b * rows, rows), rows)
            slot = (lax.broadcasted_iota(jnp.int32, (rows, 2 * cap), 1) + q * 2 * cap).astype(F32)
            total = acc[at, :]
            for j in range(2):
                sel = jnp.where(colsT[at, j:j + 1] == slot, 1.0, 0.0).astype(BF16)
                got = jnp.dot(sel[:, :cap], ret[q, 0], preferred_element_type=F32)
                got = got + jnp.dot(sel[:, cap:], ret[q, 1], preferred_element_type=F32)
                total = total + colsT[at, 2 + j:3 + j] * got
            acc[at, :] = total
            return 0

        lax.fori_loop(0, 4, block, 0)

    here(ret.at[0, other], rt_recv.at[0, other, 0])
    combine(0)
    finish(3)
    for copy in returns(3):
        copy.start()
    for q in (1, 2):
        for k in range(2):
            for b, to in enumerate((top, bottom)):
                here(ret.at[q, k, to], rt_recv.at[q, k, b])
        combine(q)
    for k in range(2):
        here(ret.at[3, k], rt_recv.at[3, k, 0])
    combine(3)
    yb[...] = acc[...].astype(BF16)

    def block_of(t):
        return pl.ds(pl.multiple_of(t * half_col, half_col), half_col)

    def gather(d):
        return remote(yb, agb.at[d - 1], ag_send.at[d - 1], ag_recv.at[d - 1], ep, lax.rem(tp + 2 * d, n_tp))

    for d in (1, 3, 2):
        gather(d).start()

    def publish(src, t, i):
        mine = pltpu.make_async_copy(src, out_hbm.at[:, block_of(t)], o_sem.at[i])
        other_core = remote(src, out_hbm.at[:, block_of(t)], p_send.at[i], p_recv.at[i], ep, partner)
        mine.start()
        other_core.start()
        return [mine, other_core]

    pending = publish(yb, tp, 0)
    for d in (1, 3, 2):
        gather(d).wait_recv()
        pending += publish(agb.at[d - 1], lax.rem(tp + n_tp - 2 * d, n_tp), d)
    for copy in pending:
        copy.wait()

    for copy in sends:
        copy.wait_send()
    here(w1.at[1], w_send.at[0])
    here(wd.at[1], w_send.at[1])
    return_own().wait_send()
    for r in range(4):
        for d in range(1, n_x):
            scatter(r, d).wait_send()
        if r:
            for copy in returns(r):
                copy.wait_send()
    for d in range(1, n_x):
        gather(d).wait_send()


def solution(mesh):
    n_ep = mesh.shape['ep']
    n_tp = mesh.shape['tp']
    row_spec = P(('dp', 'ep'), None)

    def device_body(x_loc, ids_loc, gates_loc, wg_loc, wu_loc, wd_loc):
        tokens, d_model = x_loc.shape
        n_top = ids_loc.shape[1]
        local_experts, _, ff = wg_loc.shape
        n_experts = local_experts * n_ep
        cap = CAP_NUM * n_top * tokens // (CAP_DEN * n_experts)
        n_x = n_tp // 2
        n_col = d_model // n_x
        n_tile = ff // LANES
        vmem = pltpu.VMEM
        dma = pltpu.SemaphoreType.DMA

        def kernel(*refs):
            moe_kernel(n_ep, n_tp, cap, *refs)

        any_spec = pl.BlockSpec(memory_space=pl.ANY)
        vmem_spec = pl.BlockSpec(memory_space=pltpu.VMEM)
        return pl.pallas_call(
            kernel,
            out_shape=jax.ShapeDtypeStruct((tokens, d_model), BF16),
            in_specs=[vmem_spec, vmem_spec, any_spec, any_spec, any_spec, any_spec],
            out_specs=any_spec,
            scratch_shapes=[
                vmem((tokens, d_model), BF16),
                vmem((cap, tokens), BF16),
                vmem((3, cap, d_model), BF16),
                vmem((4, cap, d_model), BF16),
                vmem((2, n_tile, d_model, 2 * LANES), BF16),
                vmem((2, ff, d_model), BF16),
                vmem((2, cap, ff), BF16),
                vmem((4, n_x, cap, n_col), BF16),
                vmem((4, n_x - 1, cap, n_col), BF16),
                vmem((4, 2, cap, n_col // 2), BF16),
                vmem((4, 2, cap, n_col // 2), BF16),
                vmem((tokens, n_col // 2), F32),
                vmem((2 * n_experts, tokens), F32),
                vmem((LANES, tokens), F32),
                vmem((tokens, LANES), F32),
                vmem((tokens, n_col // 2), BF16),
                vmem((n_x - 1, tokens, n_col // 2), BF16),
                dma((1,)), dma((4,)), dma((2,)), dma((5,)), dma((5,)),
                dma((4, n_x - 1)), dma((4, n_x - 1)), dma((4, 2, 2)), dma((4, 2, 2)),
                dma((n_x - 1,)), dma((n_x - 1,)), dma((n_x,)), dma((n_x,)), dma((n_x,)),
            ],
            compiler_params=pltpu.CompilerParams(
                collective_id=0, has_side_effects=True, vmem_limit_bytes=63 * 1024 * 1024),
        )(ids_loc.T, gates_loc.T, x_loc, wg_loc, wu_loc, wd_loc)

    return jax.shard_map(device_body, mesh=mesh,
                         in_specs=(row_spec, row_spec, row_spec, P('ep', None, 'tp'), P('ep', None, 'tp'), P('ep', 'tp', None)),
                         out_specs=row_spec, check_vma=False)
```

```python
import jax
import jax.numpy as jnp
from jax import lax
from jax.experimental import pallas as pl
from jax.experimental.pallas import tpu as pltpu
from jax.sharding import PartitionSpec as P

CAP_NUM = 5
CAP_DEN = 4
LANES = 128
MESH = pl.DeviceIdType.MESH
BF16 = jnp.bfloat16
F32 = jnp.float32


def moe_kernel(n_ep, n_tp, cap,
               ids_ref, gates_ref, x_hbm, wg_hbm, wu_hbm, wd_hbm, out,
               xv, onehot, xs, xr, w1, wd, hid, part, rv, red, ret, acc, slots, cols, colsT, sel,
               x_sem, w_sem, w_send, d_send, d_recv, rs_send, rs_recv, rt_send, rt_recv,
               ag_send, ag_recv, p_send, p_recv, both):
    tokens, d_model = x_hbm.shape
    n_x = n_tp // 2
    n_tile = w1.shape[1]
    unit = cap // 2
    ep = lax.axis_index('ep')
    tp = lax.axis_index('tp')
    core = lax.rem(tp, 2)
    other = 1 - core
    xpos = tp // 2
    partner = tp + 1 - 2 * core
    yp, y2, ym = [lax.rem(ep + i, n_ep) for i in (1, 2, 3)]
    right, left = lax.rem(tp + 2, n_tp), lax.rem(tp + n_tp - 2, n_tp)
    across = lax.rem(tp + 4, n_tp)

    def remote(src, dst, ss, rs, ep_to, tp_to):
        return pltpu.make_async_remote_copy(src_ref=src, dst_ref=dst, send_sem=ss, recv_sem=rs,
                                            device_id={'ep': ep_to, 'tp': tp_to}, device_id_type=MESH)

    def here(ref, sem):
        pltpu.make_async_copy(ref, ref, sem).wait()

    def lanes(i):
        return pl.ds(i * LANES, LANES)

    barrier = pltpu.get_barrier_semaphore()
    peers = [(ep, partner)] + [(e, t) for e in (yp, ym, y2) for t in (tp, partner)]
    peers += [(ep, t) for t in (right, across, left)]
    for e, t in peers:
        pl.semaphore_signal(barrier, inc=1, device_id={'ep': e, 'tp': t}, device_id_type=MESH)

    x_copy = pltpu.make_async_copy(x_hbm, xv, x_sem.at[0])
    x_copy.start()

    def move_weights(src, half, move):
        for i in range(n_tile):
            move(wg_hbm.at[src, :, lanes(i)], w1.at[half, i, :, pl.ds(0, LANES)], 0)
            move(wu_hbm.at[src, :, lanes(i)], w1.at[half, i, :, pl.ds(LANES, LANES)], 0)
        for h in range(2):
            for c in range(n_x):
                for k in range(2):
                    move(wd_hbm.at[src, :, lanes((c * 2 + k) * 2 + h)],
                         wd.at[half, h, c, :, pl.ds(k * LANES, LANES)], 1 + h)

    with jax.named_scope('routing'):
        n_row = slots.shape[0]
        expert = lax.broadcasted_iota(jnp.int32, (n_row, LANES), 0)
        low = lax.broadcasted_iota(jnp.int32, (LANES, LANES), 0)
        high = lax.broadcasted_iota(jnp.int32, (LANES, LANES), 1)
        before = jnp.where(low < high, 1.0, 0.0).astype(BF16)
        ones = jnp.ones((LANES, LANES), BF16)
        delta = lax.rem(expert // 2 - ep + n_ep, n_ep)
        piece = jnp.where(delta == 3, 1, jnp.where(delta == 1, 2, jnp.where(delta == 2, 3, 0)))
        base = (piece * 2 * cap + lax.rem(expert, 2) * unit + 1).astype(F32)
        carry = jnp.zeros((n_row, LANES), F32)
        cols[...] = jnp.zeros_like(cols)
        for b in range(tokens // LANES):
            span = slice(b * LANES, (b + 1) * LANES)
            hit = [expert == ids_ref[j:j + 1, span] for j in range(2)]
            mask = jnp.where(hit[0] | hit[1], 1.0, 0.0)
            rank = jnp.dot(mask.astype(BF16), before, preferred_element_type=F32) + carry
            carry = carry + jnp.dot(mask.astype(BF16), ones, preferred_element_type=F32)
            kept = rank < float(cap)
            slots[:, span] = jnp.where((mask > 0.0) & kept, rank, -1.0)
            where_to = jnp.where(kept, base + rank + jnp.where(rank < float(unit), 0.0, float(unit)), 0.0)
            for j in range(2):
                cols[j:j + 1, span] = jnp.sum(jnp.where(hit[j], where_to, 0.0), axis=0, keepdims=True) - 1.0
                cols[2 + j:3 + j, span] = gates_ref[j:j + 1, span]

    x_copy.wait()
    move_weights(core, 0, lambda src, dst, i: pltpu.make_async_copy(src, dst, w_sem.at[0, i]).start())


    def pick(expert_id, dst):
        with jax.named_scope('pick'):
            row = slots[pl.ds(expert_id, 1), :]
            slot = lax.broadcasted_iota(jnp.int32, (cap, tokens), 0).astype(F32)
            onehot[...] = jnp.where(slot == row, 1.0, 0.0).astype(BF16)
            step = 512
            for c in range(d_model // step):
                got = jnp.dot(onehot[...], xv[:, c * step:(c + 1) * step], preferred_element_type=F32).astype(BF16)
                for u in range(2):
                    dst[u, :, c * step:(c + 1) * step] = got[u * unit:(u + 1) * unit]

    def send_rows(i, u, land, to):
        return remote(xs.at[i, u], xr.at[land], d_send.at[i, u], d_recv.at[land], to, tp)

    near = [[send_rows(0, 0, 3, yp), send_rows(0, 1, 5, yp)], [send_rows(1, 0, 2, ym), send_rows(1, 1, 4, ym)]]
    far = [send_rows(2, 0, 6, y2), send_rows(2, 1, 7, y2)]
    pick(2 * yp + core, xs.at[0])
    with jax.named_scope('barrier'):
        pl.semaphore_wait(barrier, len(peers))
    for copy in near[0]:
        copy.start()
    move_weights(other, 1, lambda src, dst, i: remote(src, dst, w_send.at[i], w_sem.at[1, i], ep, partner).start())
    pick(2 * ym + core, xs.at[1])
    for copy in near[1]:
        copy.start()
    pick(2 * ep + core, xr.at[pl.ds(0, 2)])

    def scatter(g, u, n, h, d):
        c = lax.rem(xpos + d, n_x)
        at = pl.ds(u, n)
        return remote(part.at[at, h, c], rv.at[at, h, d - 1], rs_send.at[g, h, d - 1], rs_recv.at[g, h, d - 1],
                      ep, 2 * c + core)

    def ffn(g, u, n, first):
        rows = n * unit
        at = pl.ds(u, n)

        def gate_up(half, _):
            if first is not None:
                @pl.when(first)
                def _():
                    with jax.named_scope('wait_w1'):
                        here(w1.at[half], w_sem.at[half, 0])
            with jax.named_scope('gate_up'):
                for i in range(n_tile):
                    ab = jnp.dot(xr[at].reshape(rows, d_model), w1[half, i], preferred_element_type=F32)
                    a, b = ab[:, :LANES], ab[:, LANES:]
                    hid[half, 0:rows, i * LANES:(i + 1) * LANES] = (jax.nn.silu(a) * b).astype(BF16)
            return 0

        lax.fori_loop(0, 2, gate_up, 0)

        def down(h, _):
            if first is not None:
                @pl.when(first)
                def _():
                    with jax.named_scope('wait_wd'):
                        for half in range(2):
                            here(wd.at[half, h], w_sem.at[half, 1 + h])
            with jax.named_scope('down'):
                for c in range(n_x):
                    o = jnp.dot(hid[0, 0:rows], wd[0, h, c], preferred_element_type=F32)
                    o = o + jnp.dot(hid[1, 0:rows], wd[1, h, c], preferred_element_type=F32)
                    part[at, h, c] = o.astype(BF16).reshape(n, unit, 2 * LANES)
                for d in range(1, n_x):
                    scatter(g, u, n, h, d).start()
            return 0

        lax.fori_loop(0, 2, down, 0)

    def total(g, u, n, h):
        with jax.named_scope('wait_rs'):
            for d in range(1, n_x):
                scatter(g, u, n, h, d).wait_recv()
        with jax.named_scope('total'):
            for i in range(n):
                t = part[u + i, h, xpos].astype(F32)
                for d in range(1, n_x):
                    t = t + rv[u + i, h, d - 1].astype(F32)
                t = t.astype(BF16)
                for k in range(2):
                    red[u + i, h, k] = t[:, k * LANES:(k + 1) * LANES]

    back = {2: (yp, 1, 0), 3: (ym, 2, 0), 4: (yp, 1, 1), 5: (ym, 2, 1), 6: (y2, 3, 0), 7: (y2, 3, 1)}

    def returns(u, h):
        to, q, b = back[u]
        return [remote(red.at[u, h, k], ret.at[h, q, b, core], rt_send.at[u, h, k], rt_recv.at[h, q, b, core],
                       to, 2 * xpos + k) for k in range(2)]

    def return_own(h):
        return [remote(red.at[b, h, other], ret.at[h, 0, b, core], rt_send.at[b, h, 0], rt_recv.at[h, 0, b, core],
                       ep, partner) for b in range(2)]

    def chunk(r, _):
        for q in (1, 2):
            @pl.when(r == q)
            def _():
                with jax.named_scope('wait_rows'):
                    for u in (2 * q, 2 * q + 1):
                        here(xr.at[u], d_recv.at[u])

        ffn(r, 2 * r, 2, r == 0)

        @pl.when(r == 0)
        def _():
            pick(2 * y2 + core, xs.at[2])
            for b in range(tokens // LANES):
                colsT[b * LANES:(b + 1) * LANES, :] = cols[:, b * LANES:(b + 1) * LANES].T

        @pl.when(r == 1)
        def _():
            with jax.named_scope('near_done'):
                for copy in near[0] + near[1]:
                    copy.wait_send()
                pl.semaphore_signal(both, inc=1, device_id={'ep': ep, 'tp': partner}, device_id_type=MESH)
                pl.semaphore_wait(both, 1)
            for copy in far:
                copy.start()

        @pl.when(r > 0)
        def _():
            for h in range(2):
                total(r - 1, 2 * r - 2, 2, h)

        @pl.when(r == 1)
        def _():
            for h in range(2):
                for copy in return_own(h):
                    copy.start()
                for b in range(2):
                    ret[h, 0, b, core] = red[b, h, core]

        @pl.when(r == 2)
        def _():
            for h in range(2):
                for u in (2, 3):
                    for copy in returns(u, h):
                        copy.start()
        return 0

    lax.fori_loop(0, 3, chunk, 0)

    rows = tokens // 4
    span = 2 * unit

    def choose(at, j, first_slot, n):
        slot = (lax.broadcasted_iota(jnp.int32, (rows, n), 1) + first_slot).astype(F32)
        return jnp.where(colsT[at, j:j + 1] == slot, 1.0, 0.0).astype(BF16)

    def combine(q, b, n, fresh):
        with jax.named_scope('combine'):
            def block(i, _):
                at = pl.ds(pl.multiple_of(i * rows, rows), rows)
                t = jnp.zeros((rows, 2 * LANES), F32) if fresh else acc[at, :]
                y = jnp.concatenate([ret[h, q, pl.ds(b, n)].reshape(n * span, LANES) for h in range(2)], axis=1)
                for j in range(2):
                    got = jnp.dot(choose(at, j, q * 2 * cap + b * span, n * span), y, preferred_element_type=F32)
                    t = t + colsT[at, 2 + j:3 + j] * got
                acc[at, :] = t
                return 0

            lax.fori_loop(0, 4, block, 0)

    def wait_ret(h, q, b):
        with jax.named_scope('wait_ret'):
            for k in range(2):
                here(ret.at[h, q, b, k], rt_recv.at[h, q, b, k])

    with jax.named_scope('wait_own'):
        for h in range(2):
            for b in range(2):
                here(ret.at[h, 0, b, other], rt_recv.at[h, 0, b, other])
    combine(0, 0, 2, True)

    def tail(i, _):
        u = 6 + i
        with jax.named_scope('wait_rows'):
            here(xr.at[u], d_recv.at[u])
        ffn(3 + i, u, 1, None)

        @pl.when(i == 0)
        def _():
            for h in range(2):
                total(2, 4, 2, h)
                for w in (4, 5):
                    for copy in returns(w, h):
                        copy.start()
        return 0

    lax.fori_loop(0, 2, tail, 0)
    for h in range(2):
        total(3, 6, 1, h)
        for copy in returns(6, h):
            copy.start()

    def pick_last(i, _):
        at = pl.ds(pl.multiple_of(i * rows, rows), rows)
        for j in range(2):
            sel[j, at, :] = choose(at, j, 3 * 2 * cap + span, span)
        return 0

    lax.fori_loop(0, 4, pick_last, 0)
    for q in (1, 2):
        for h in range(2):
            for b in range(2):
                wait_ret(h, q, b)
        combine(q, 0, 2, False)
    for h in range(2):
        total(4, 7, 1, h)
        for copy in returns(7, h):
            copy.start()
    for h in range(2):
        wait_ret(h, 3, 0)
    combine(3, 0, 1, False)

    half_rows = tokens // 2

    def place(t, h, p):
        at = slice(None) if p is None else pl.ds(p * half_rows, half_rows)
        return out.at[at, pl.ds(pl.multiple_of((2 * t + h) * LANES, LANES), LANES)]

    def spread(t, h, p, to, i):
        return remote(place(t, h, p), place(t, h, p), ag_send.at[h, i], ag_recv.at[h, i], ep, to)

    def publish(t, h, p, i):
        return remote(place(t, h, p), place(t, h, p), p_send.at[h, i], p_recv.at[h, i], ep, partner)

    started = []

    def go(copy):
        copy.start()
        started.append(copy)

    for h in range(2):
        wait_ret(h, 3, 1)
        with jax.named_scope('last'):
            y = ret[h, 3, 1].reshape(span, LANES)
            for i in range(4):
                at = slice(i * rows, (i + 1) * rows)
                t = acc[at, h * LANES:(h + 1) * LANES]
                for j in range(2):
                    got = jnp.dot(sel[j, at, :], y, preferred_element_type=F32)
                    t = t + colsT[at, 2 + j:3 + j] * got
                out[at, pl.ds(pl.multiple_of((2 * tp + h) * LANES, LANES), LANES)] = t.astype(BF16)
        go(spread(tp, h, 0, right, 0))
        go(spread(tp, h, 1, left, 3))
        go(spread(tp, h, 1, right, 1))
        go(spread(tp, h, 0, left, 2))
        go(publish(tp, h, None, 0))
    with jax.named_scope('gather'):
        for h in range(2):
            spread(left, h, 0, right, 0).wait_recv()
            go(spread(left, h, 0, right, 4))
            spread(right, h, 1, left, 3).wait_recv()
            go(spread(right, h, 1, left, 5))
            go(publish(left, h, 0, 1))
            go(publish(right, h, 1, 2))
        for h in range(2):
            spread(left, h, 1, right, 1).wait_recv()
            go(publish(left, h, 1, 3))
            spread(right, h, 0, left, 2).wait_recv()
            go(publish(right, h, 0, 4))
        for h in range(2):
            spread(across, h, 0, right, 4).wait_recv()
            go(publish(across, h, 0, 5))
            spread(across, h, 1, left, 5).wait_recv()
            go(publish(across, h, 1, 6))
        for h in range(2):
            for i in range(7):
                publish(tp, h, None if i == 0 else 0, i).wait_recv()

    with jax.named_scope('drain'):
        for copy in far + started:
            copy.wait_send()
        here(w1.at[1], w_send.at[0])
        for h in range(2):
            here(wd.at[1, h], w_send.at[1 + h])
        for h in range(2):
            for copy in return_own(h):
                copy.wait_send()
            for u in back:
                for copy in returns(u, h):
                    copy.wait_send()
            for d in range(1, n_x):
                for g in range(3):
                    scatter(g, 2 * g, 2, h, d).wait_send()
                for i in range(2):
                    scatter(3 + i, 6 + i, 1, h, d).wait_send()


def solution(mesh):
    n_ep = mesh.shape['ep']
    n_tp = mesh.shape['tp']
    row_spec = P(('dp', 'ep'), None)

    def device_body(x_loc, ids_loc, gates_loc, wg_loc, wu_loc, wd_loc):
        tokens, d_model = x_loc.shape
        n_top = ids_loc.shape[1]
        local_experts, _, ff = wg_loc.shape
        n_experts = local_experts * n_ep
        cap = CAP_NUM * n_top * tokens // (CAP_DEN * n_experts)
        unit = cap // 2
        n_x = n_tp // 2
        n_tile = ff // LANES
        vmem = pltpu.VMEM
        dma = pltpu.SemaphoreType.DMA

        def kernel(*refs):
            moe_kernel(n_ep, n_tp, cap, *refs)

        any_spec = pl.BlockSpec(memory_space=pl.ANY)
        vmem_spec = pl.BlockSpec(memory_space=pltpu.VMEM)
        return pl.pallas_call(
            kernel,
            out_shape=pltpu.VMEM((tokens, d_model), BF16),
            in_specs=[vmem_spec, vmem_spec, any_spec, any_spec, any_spec, any_spec],
            out_specs=vmem_spec,
            scratch_shapes=[
                vmem((tokens, d_model), BF16),
                vmem((cap, tokens), BF16),
                vmem((3, 2, unit, d_model), BF16),
                vmem((8, unit, d_model), BF16),
                vmem((2, n_tile, d_model, 2 * LANES), BF16),
                vmem((2, 2, n_x, ff, 2 * LANES), BF16),
                vmem((2, cap, ff), BF16),
                vmem((8, 2, n_x, unit, 2 * LANES), BF16),
                vmem((8, 2, n_x - 1, unit, 2 * LANES), BF16),
                vmem((8, 2, 2, unit, LANES), BF16),
                vmem((2, 4, 2, 2, unit, LANES), BF16),
                vmem((tokens, 2 * LANES), F32),
                vmem((2 * n_experts, tokens), F32),
                vmem((LANES, tokens), F32),
                vmem((tokens, LANES), F32),
                vmem((2, tokens, 2 * unit), BF16),
                dma((1,)), dma((2, 3)), dma((3,)), dma((3, 2)), dma((8,)),
                dma((5, 2, n_x - 1)), dma((5, 2, n_x - 1)), dma((8, 2, 2)), dma((2, 4, 2, 2)),
                dma((2, 6)), dma((2, 6)), dma((2, 7)), dma((2, 7)), pltpu.SemaphoreType.REGULAR,
            ],
            compiler_params=pltpu.CompilerParams(
                collective_id=0, has_side_effects=True, vmem_limit_bytes=58 * 1024 * 1024),
        )(ids_loc.T, gates_loc.T, x_loc, wg_loc, wu_loc, wd_loc)

    return jax.shard_map(device_body, mesh=mesh,
                         in_specs=(row_spec, row_spec, row_spec, P('ep', None, 'tp'), P('ep', None, 'tp'), P('ep', 'tp', None)),
                         out_specs=row_spec, check_vma=False)
```

```python
import jax
import jax.numpy as jnp
from jax import lax
from jax.experimental import pallas as pl
from jax.experimental.pallas import tpu as pltpu
from jax.sharding import PartitionSpec as P

CAP_NUM = 5
CAP_DEN = 4
LANES = 128
MESH = pl.DeviceIdType.MESH
BF16 = jnp.bfloat16
F32 = jnp.float32


def moe_kernel(n_ep, n_tp, cap,
               ids_hbm, gates_hbm, x_hbm, wg_hbm, wu_hbm, wd_hbm, out,
               ids_ref, gates_ref, xv, onehot, xs, xr, w1, wd, hid, part, rv, red, ret, acc, slots, cols, colsT, sel,
               x_sem, w_sem, w_send, d_send, d_recv, rs_send, rs_recv, rt_send, rt_recv,
               ag_send, ag_recv, p_send, p_recv, f_send, f_recv, both):
    tokens, d_model = x_hbm.shape
    n_x = n_tp // 2
    n_tile = w1.shape[1]
    unit = cap // 2
    ep = lax.axis_index('ep')
    tp = lax.axis_index('tp')
    core = lax.rem(tp, 2)
    other = 1 - core
    xpos = tp // 2
    partner = tp + 1 - 2 * core
    yp, y2, ym = [lax.rem(ep + i, n_ep) for i in (1, 2, 3)]
    right, left = lax.rem(tp + 2, n_tp), lax.rem(tp + n_tp - 2, n_tp)
    across = lax.rem(tp + 4, n_tp)

    def remote(src, dst, ss, rs, ep_to, tp_to):
        return pltpu.make_async_remote_copy(src_ref=src, dst_ref=dst, send_sem=ss, recv_sem=rs,
                                            device_id={'ep': ep_to, 'tp': tp_to}, device_id_type=MESH)

    def here(ref, sem):
        pltpu.make_async_copy(ref, ref, sem).wait()

    def lanes(i):
        return pl.ds(i * LANES, LANES)

    barrier = pltpu.get_barrier_semaphore()
    peers = [(ep, partner)] + [(e, t) for e in (yp, ym, y2) for t in (tp, partner)]
    peers += [(ep, t) for t in (right, across, left)]
    for e, t in peers:
        pl.semaphore_signal(barrier, inc=1, device_id={'ep': e, 'tp': t}, device_id_type=MESH)

    x_copy = pltpu.make_async_copy(x_hbm, xv, x_sem.at[0])
    x_copy.start()
    small = [pltpu.make_async_copy(ids_hbm, ids_ref, x_sem.at[1]), pltpu.make_async_copy(gates_hbm, gates_ref, x_sem.at[2])]
    for copy in small:
        copy.start()

    def move_weights(src, half, move):
        for i in range(n_tile):
            move(wg_hbm.at[src, :, lanes(i)], w1.at[half, i, :, pl.ds(0, LANES)], 0)
            move(wu_hbm.at[src, :, lanes(i)], w1.at[half, i, :, pl.ds(LANES, LANES)], 0)
        for h in range(2):
            for c in range(n_x):
                for k in range(2):
                    move(wd_hbm.at[src, :, lanes((c * 2 + k) * 2 + h)],
                         wd.at[half, h, c, :, pl.ds(k * LANES, LANES)], 1 + h)

    for copy in small:
        copy.wait()
    with jax.named_scope('routing'):
        n_row = slots.shape[0]
        expert = lax.broadcasted_iota(jnp.int32, (n_row, LANES), 0)
        low = lax.broadcasted_iota(jnp.int32, (LANES, LANES), 0)
        high = lax.broadcasted_iota(jnp.int32, (LANES, LANES), 1)
        before = jnp.where(low < high, 1.0, 0.0).astype(BF16)
        ones = jnp.ones((LANES, LANES), BF16)
        delta = lax.rem(expert // 2 - ep + n_ep, n_ep)
        piece = jnp.where(delta == 3, 1, jnp.where(delta == 1, 2, jnp.where(delta == 2, 3, 0)))
        base = (piece * 2 * cap + lax.rem(expert, 2) * unit + 1).astype(F32)
        carry = jnp.zeros((n_row, LANES), F32)
        cols[...] = jnp.zeros_like(cols)
        for b in range(tokens // LANES):
            span = slice(b * LANES, (b + 1) * LANES)
            hit = [expert == ids_ref[j:j + 1, span] for j in range(2)]
            mask = jnp.where(hit[0] | hit[1], 1.0, 0.0)
            rank = jnp.dot(mask.astype(BF16), before, preferred_element_type=F32) + carry
            carry = carry + jnp.dot(mask.astype(BF16), ones, preferred_element_type=F32)
            kept = rank < float(cap)
            slots[:, span] = jnp.where((mask > 0.0) & kept, rank, -1.0)
            where_to = jnp.where(kept, base + rank + jnp.where(rank < float(unit), 0.0, float(unit)), 0.0)
            for j in range(2):
                cols[j:j + 1, span] = jnp.sum(jnp.where(hit[j], where_to, 0.0), axis=0, keepdims=True) - 1.0
                cols[2 + j:3 + j, span] = gates_ref[j:j + 1, span]

    x_copy.wait()
    move_weights(core, 0, lambda src, dst, i: pltpu.make_async_copy(src, dst, w_sem.at[0, i]).start())


    def pick(expert_id, dst):
        with jax.named_scope('pick'):
            row = slots[pl.ds(expert_id, 1), :]
            slot = lax.broadcasted_iota(jnp.int32, (cap, tokens), 0).astype(F32)
            onehot[...] = jnp.where(slot == row, 1.0, 0.0).astype(BF16)
            step = 512
            for c in range(d_model // step):
                got = jnp.dot(onehot[...], xv[:, c * step:(c + 1) * step], preferred_element_type=F32).astype(BF16)
                for u in range(2):
                    dst[u, :, c * step:(c + 1) * step] = got[u * unit:(u + 1) * unit]

    def send_rows(i, u, land, to):
        return remote(xs.at[i, u], xr.at[land], d_send.at[i, u], d_recv.at[land], to, tp)

    quarter = d_model // 4
    parity = lax.rem(xpos, 2)

    def columns(q):
        return pl.ds(pl.multiple_of((2 * parity + q) * quarter, quarter), quarter)

    mine = pl.ds(pl.multiple_of(2 * parity * quarter, 2 * quarter), 2 * quarter)

    def send_half(i, land, to):
        return remote(xs.at[i, 0, :, mine], xr.at[land, :, mine], d_send.at[i, 0], d_recv.at[land], to, tp)

    def forward(u, q, to):
        return remote(xr.at[u, :, columns(q)], xr.at[u, :, columns(q)], f_send.at[u - 2, q], f_recv.at[u - 2, q], ep, to)

    near = [[send_half(0, 3, yp), send_rows(0, 1, 5, yp)], [send_half(1, 2, ym), send_rows(1, 1, 4, ym)]]
    far = [send_rows(2, 0, 6, y2), send_rows(2, 1, 7, y2)]
    pick(2 * yp + core, xs.at[0])
    with jax.named_scope('barrier'):
        pl.semaphore_wait(barrier, len(peers))
    for copy in near[0]:
        copy.start()
    move_weights(other, 1, lambda src, dst, i: remote(src, dst, w_send.at[i], w_sem.at[1, i], ep, partner).start())
    pick(2 * ym + core, xs.at[1])
    for copy in near[1]:
        copy.start()
    pick(2 * ep + core, xr.at[pl.ds(0, 2)])

    def scatter(g, u, n, h, d):
        c = lax.rem(xpos + d, n_x)
        at = pl.ds(u, n)
        return remote(part.at[at, h, c], rv.at[at, h, d - 1], rs_send.at[g, h, d - 1], rs_recv.at[g, h, d - 1],
                      ep, 2 * c + core)

    def total(g, u, n, h):
        with jax.named_scope('wait_rs'):
            for d in range(1, n_x):
                scatter(g, u, n, h, d).wait_recv()
        with jax.named_scope('total'):
            for i in range(n):
                t = part[u + i, h, xpos].astype(F32)
                for d in range(1, n_x):
                    t = t + rv[u + i, h, d - 1].astype(F32)
                t = t.astype(BF16)
                for k in range(2):
                    red[u + i, h, k] = t[:, k * LANES:(k + 1) * LANES]

    back = {2: (yp, 1, 0), 3: (ym, 2, 0), 4: (yp, 1, 1), 5: (ym, 2, 1), 6: (y2, 3, 0), 7: (y2, 3, 1)}

    def returns(u, h):
        to, q, b = back[u]
        return [remote(red.at[u, h, k], ret.at[h, q, b, core], rt_send.at[u, h, k], rt_recv.at[h, q, b, core],
                       to, 2 * xpos + k) for k in range(2)]

    def ffn(g, u, n, first=None, send=True, also=None):
        rows = n * unit
        at = pl.ds(u, n)

        def gate_up(half, _):
            with jax.named_scope('gate_up'):
                for i in range(n_tile):
                    ab = jnp.dot(xr[at].reshape(rows, d_model), w1[half, i], preferred_element_type=F32)
                    a, b = ab[:, :LANES], ab[:, LANES:]
                    hid[half, 0:rows, i * LANES:(i + 1) * LANES] = (jax.nn.silu(a) * b).astype(BF16)
            return 0

        if first is None:
            lax.fori_loop(0, 2, gate_up, 0)
        else:
            for half in range(2):
                with jax.named_scope('wait_w1'):
                    here(w1.at[half], w_sem.at[half, 0])
                gate_up(half, 0)
                if half == 0:
                    first()

        def down(h, _):
            if first:
                with jax.named_scope('wait_wd'):
                    for half in range(2):
                        here(wd.at[half, h], w_sem.at[half, 1 + h])
            with jax.named_scope('down'):
                for c in range(n_x):
                    o = jnp.dot(hid[0, 0:rows], wd[0, h, c], preferred_element_type=F32)
                    o = o + jnp.dot(hid[1, 0:rows], wd[1, h, c], preferred_element_type=F32)
                    part[at, h, c] = o.astype(BF16).reshape(n, unit, 2 * LANES)
                if send:
                    for d in range(1, n_x):
                        scatter(g, u, n, h, d).start()
                if also is not None:
                    @pl.when(also)
                    def _():
                        for d in range(1, n_x):
                            scatter(6, 1, 1, h, d).start()

                    @pl.when(also & (h == 0))
                    def _():
                        for k in range(2):
                            total(4, 6, 1, k)
                            for copy in returns(6, k):
                                copy.start()
            return 0

        lax.fori_loop(0, 2, down, 0)

    def return_own(b, h):
        return remote(red.at[b, h, other], ret.at[h, 0, b, core], rt_send.at[b, h, 0], rt_recv.at[h, 0, b, core],
                      ep, partner)

    def keep_own(b, h):
        return_own(b, h).start()
        ret[h, 0, b, core] = red[b, h, core]

    def between():
        pick(2 * y2 + core, xs.at[2])
        for b in range(tokens // LANES):
            colsT[b * LANES:(b + 1) * LANES, :] = cols[:, b * LANES:(b + 1) * LANES].T
        with jax.named_scope('forward'):
            for u in (2, 3):
                here(xr.at[u, :, mine], d_recv.at[u])
                forward(u, 0, right).start()
                forward(u, 1, left).start()

    ffn(0, 0, 1, first=between)

    def near_unit(i, _):
        u = 2 + i
        with jax.named_scope('wait_rows'):
            for q in range(2):
                here(xr.at[u, :, columns(q)], f_recv.at[i, q])
        ffn(1 + i, u, 1)

        @pl.when(i == 0)
        def _():
            with jax.named_scope('near_done'):
                for copy in near[0] + near[1]:
                    copy.wait_send()
                pl.semaphore_signal(both, inc=1, device_id={'ep': ep, 'tp': partner}, device_id_type=MESH)
                pl.semaphore_wait(both, 1)
            for copy in far:
                copy.start()

        @pl.when(i == 1)
        def _():
            for h in range(2):
                total(0, 0, 1, h)
                keep_own(0, h)
        return 0

    lax.fori_loop(0, 2, near_unit, 0)
    with jax.named_scope('wait_rows'):
        for u in (4, 5):
            here(xr.at[u], d_recv.at[u])
    ffn(3, 4, 2)
    ffn(6, 1, 1, send=False)
    for u in (2, 3):
        for h in range(2):
            total(u - 1, u, 1, h)
            for copy in returns(u, h):
                copy.start()

    rows = tokens // 4
    span = 2 * unit

    def choose(at, j, first_slot, n):
        slot = (lax.broadcasted_iota(jnp.int32, (rows, n), 1) + first_slot).astype(F32)
        return jnp.where(colsT[at, j:j + 1] == slot, 1.0, 0.0).astype(BF16)

    def combine(q, b, n, fresh):
        with jax.named_scope('combine'):
            def block(i, _):
                at = pl.ds(pl.multiple_of(i * rows, rows), rows)
                t = jnp.zeros((rows, 2 * LANES), F32) if fresh else acc[at, :]
                y = jnp.concatenate([ret[h, q, pl.ds(b, n)].reshape(n * span, LANES) for h in range(2)], axis=1)
                for j in range(2):
                    got = jnp.dot(choose(at, j, q * 2 * cap + b * span, n * span), y, preferred_element_type=F32)
                    t = t + colsT[at, 2 + j:3 + j] * got
                acc[at, :] = t
                return 0

            lax.fori_loop(0, 4, block, 0)

    def wait_ret(h, q, b):
        with jax.named_scope('wait_ret'):
            for k in range(2):
                here(ret.at[h, q, b, k], rt_recv.at[h, q, b, k])

    def wait_own(h, b):
        with jax.named_scope('wait_own'):
            here(ret.at[h, 0, b, other], rt_recv.at[h, 0, b, other])

    for h in range(2):
        wait_own(h, 0)
    combine(0, 0, 1, True)

    def pick_last(i, _):
        at = pl.ds(pl.multiple_of(i * rows, rows), rows)
        for j in range(2):
            for w, q in enumerate((3, 0)):
                sel[j, at, w * span:(w + 1) * span] = choose(at, j, q * 2 * cap + span, span)
        return 0

    def tail(i, _):
        u = 6 + i
        with jax.named_scope('wait_rows'):
            here(xr.at[u], d_recv.at[u])
        ffn(4 + i, u, 1, also=i == 1)

        @pl.when(i == 0)
        def _():
            lax.fori_loop(0, 4, pick_last, 0)
            for h in range(2):
                total(3, 4, 2, h)
                for w in (4, 5):
                    for copy in returns(w, h):
                        copy.start()
        return 0

    lax.fori_loop(0, 2, tail, 0)

    def combine_near(q):
        for h in range(2):
            for b in range(2):
                wait_ret(h, q, b)
        combine(q, 0, 2, False)

    def last_far(h):
        total(5, 7, 1, h)
        for copy in returns(7, h):
            copy.start()

    def last_own(h):
        total(6, 1, 1, h)
        keep_own(1, h)

    combine_near(1)
    last_far(0)
    combine_near(2)
    last_own(0)
    last_far(1)
    for h in range(2):
        wait_ret(h, 3, 0)
    combine(3, 0, 1, False)

    half_rows = tokens // 2

    def place(t, h, p):
        at = slice(None) if p is None else pl.ds(p * half_rows, half_rows)
        return out.at[at, pl.ds(pl.multiple_of((2 * t + h) * LANES, LANES), LANES)]

    def spread(t, h, p, to, i):
        return remote(place(t, h, p), place(t, h, p), ag_send.at[h, i], ag_recv.at[h, i], ep, to)

    def publish(t, h, p, i):
        return remote(place(t, h, p), place(t, h, p), p_send.at[h, i], p_recv.at[h, i], ep, partner)

    started = []

    def go(copy):
        copy.start()
        started.append(copy)

    def finish(h):
        wait_own(h, 1)
        wait_ret(h, 3, 1)
        with jax.named_scope('last'):
            y = jnp.concatenate([ret[h, 3, 1].reshape(span, LANES), ret[h, 0, 1].reshape(span, LANES)], axis=0)
            for i in range(4):
                at = slice(i * rows, (i + 1) * rows)
                t = acc[at, h * LANES:(h + 1) * LANES]
                for j in range(2):
                    got = jnp.dot(sel[j, at, :], y, preferred_element_type=F32)
                    t = t + colsT[at, 2 + j:3 + j] * got
                out[at, pl.ds(pl.multiple_of((2 * tp + h) * LANES, LANES), LANES)] = t.astype(BF16)
        go(spread(tp, h, 0, right, 0))
        go(spread(tp, h, 1, left, 3))
        go(spread(tp, h, 1, right, 1))
        go(spread(tp, h, 0, left, 2))
        go(publish(tp, h, None, 0))

    def relay(h):
        with jax.named_scope('relay'):
            spread(left, h, 0, right, 0).wait_recv()
            go(spread(left, h, 0, right, 4))
            spread(right, h, 1, left, 3).wait_recv()
            go(spread(right, h, 1, left, 5))
            go(publish(left, h, 0, 1))
            go(publish(right, h, 1, 2))

    finish(0)
    last_own(1)
    finish(1)
    relay(0)
    relay(1)
    with jax.named_scope('gather'):
        for h in range(2):
            spread(left, h, 1, right, 1).wait_recv()
            go(publish(left, h, 1, 3))
            spread(right, h, 0, left, 2).wait_recv()
            go(publish(right, h, 0, 4))
        for h in range(2):
            spread(across, h, 0, right, 4).wait_recv()
            go(publish(across, h, 0, 5))
            spread(across, h, 1, left, 5).wait_recv()
            go(publish(across, h, 1, 6))
        for h in range(2):
            for i in range(7):
                publish(tp, h, None if i == 0 else 0, i).wait_recv()

    with jax.named_scope('drain'):
        for copy in far + started:
            copy.wait_send()
        here(w1.at[1], w_send.at[0])
        for u in (2, 3):
            forward(u, 0, right).wait_send()
            forward(u, 1, left).wait_send()
        for h in range(2):
            here(wd.at[1, h], w_send.at[1 + h])
        for h in range(2):
            for b in range(2):
                return_own(b, h).wait_send()
            for u in back:
                for copy in returns(u, h):
                    copy.wait_send()
            for d in range(1, n_x):
                for g, u, n in ((0, 0, 1), (1, 2, 1), (2, 3, 1), (3, 4, 2), (4, 6, 1), (5, 7, 1), (6, 1, 1)):
                    scatter(g, u, n, h, d).wait_send()


def solution(mesh):
    n_ep = mesh.shape['ep']
    n_tp = mesh.shape['tp']
    row_spec = P(('dp', 'ep'), None)

    def device_body(x_loc, ids_loc, gates_loc, wg_loc, wu_loc, wd_loc):
        tokens, d_model = x_loc.shape
        n_top = ids_loc.shape[1]
        local_experts, _, ff = wg_loc.shape
        n_experts = local_experts * n_ep
        cap = CAP_NUM * n_top * tokens // (CAP_DEN * n_experts)
        unit = cap // 2
        n_x = n_tp // 2
        n_tile = ff // LANES
        vmem = pltpu.VMEM
        dma = pltpu.SemaphoreType.DMA

        def kernel(*refs):
            moe_kernel(n_ep, n_tp, cap, *refs)

        any_spec = pl.BlockSpec(memory_space=pl.ANY)
        vmem_spec = pl.BlockSpec(memory_space=pltpu.VMEM)
        return pl.pallas_call(
            kernel,
            out_shape=pltpu.VMEM((tokens, d_model), BF16),
            in_specs=[any_spec] * 6,
            out_specs=vmem_spec,
            scratch_shapes=[
                vmem(ids_loc.shape[::-1], jnp.int32),
                vmem(gates_loc.shape[::-1], F32),
                vmem((tokens, d_model), BF16),
                vmem((cap, tokens), BF16),
                vmem((3, 2, unit, d_model), BF16),
                vmem((8, unit, d_model), BF16),
                vmem((2, n_tile, d_model, 2 * LANES), BF16),
                vmem((2, 2, n_x, ff, 2 * LANES), BF16),
                vmem((2, cap, ff), BF16),
                vmem((8, 2, n_x, unit, 2 * LANES), BF16),
                vmem((8, 2, n_x - 1, unit, 2 * LANES), BF16),
                vmem((8, 2, 2, unit, LANES), BF16),
                vmem((2, 4, 2, 2, unit, LANES), BF16),
                vmem((tokens, 2 * LANES), F32),
                vmem((2 * n_experts, tokens), F32),
                vmem((LANES, tokens), F32),
                vmem((tokens, LANES), F32),
                vmem((2, tokens, 4 * unit), BF16),
                dma((3,)), dma((2, 3)), dma((3,)), dma((3, 2)), dma((8,)),
                dma((7, 2, n_x - 1)), dma((7, 2, n_x - 1)), dma((8, 2, 2)), dma((2, 4, 2, 2)),
                dma((2, 6)), dma((2, 6)), dma((2, 7)), dma((2, 7)), dma((2, 2)), dma((2, 2)),
                pltpu.SemaphoreType.REGULAR,
            ],
            compiler_params=pltpu.CompilerParams(
                collective_id=0, has_side_effects=True, vmem_limit_bytes=58 * 1024 * 1024),
        )(ids_loc.T, gates_loc.T, x_loc, wg_loc, wu_loc, wd_loc)

    return jax.shard_map(device_body, mesh=mesh,
                         in_specs=(row_spec, row_spec, row_spec, P('ep', None, 'tp'), P('ep', None, 'tp'), P('ep', 'tp', None)),
                         out_specs=row_spec, check_vma=False)
```

```python
import jax
import jax.numpy as jnp
from jax import lax
from jax.experimental import pallas as pl
from jax.experimental.pallas import tpu as pltpu
from jax.sharding import PartitionSpec as P

CAP_NUM = 5
CAP_DEN = 4
LANES = 128
MESH = pl.DeviceIdType.MESH
BF16 = jnp.bfloat16
F32 = jnp.float32


def moe_kernel(n_ep, n_tp, cap,
               ids_hbm, gates_hbm, x_hbm, wg_hbm, wu_hbm, wd_hbm, out,
               ids_ref, gates_ref, xv, onehot, xs, xr, w1, wd, hid, part, rv, red, ret, acc, slots, cols, colsT, sel,
               x_sem, w_sem, w_send, d_send, d_recv, rs_send, rs_recv, rt_send, rt_recv,
               ag_send, ag_recv, p_send, p_recv, f_send, f_recv, h_send, h_recv, both):
    tokens, d_model = x_hbm.shape
    n_x = n_tp // 2
    n_tile = w1.shape[1]
    unit = cap // 2
    ep = lax.axis_index('ep')
    tp = lax.axis_index('tp')
    core = lax.rem(tp, 2)
    other = 1 - core
    xpos = tp // 2
    partner = tp + 1 - 2 * core
    yp, y2, ym = [lax.rem(ep + i, n_ep) for i in (1, 2, 3)]
    right, left = lax.rem(tp + 2, n_tp), lax.rem(tp + n_tp - 2, n_tp)
    across = lax.rem(tp + 4, n_tp)

    def remote(src, dst, ss, rs, ep_to, tp_to):
        return pltpu.make_async_remote_copy(src_ref=src, dst_ref=dst, send_sem=ss, recv_sem=rs,
                                            device_id={'ep': ep_to, 'tp': tp_to}, device_id_type=MESH)

    def here(ref, sem):
        pltpu.make_async_copy(ref, ref, sem).wait()

    def lanes(i):
        return pl.ds(i * LANES, LANES)

    barrier = pltpu.get_barrier_semaphore()
    peers = [(ep, partner)] + [(e, t) for e in (yp, ym, y2) for t in (tp, partner)]
    peers += [(ep, t) for t in (right, across, left)]
    for e, t in peers:
        pl.semaphore_signal(barrier, inc=1, device_id={'ep': e, 'tp': t}, device_id_type=MESH)

    x_copy = pltpu.make_async_copy(x_hbm, xv, x_sem.at[0])
    x_copy.start()
    small = [pltpu.make_async_copy(ids_hbm, ids_ref, x_sem.at[1]), pltpu.make_async_copy(gates_hbm, gates_ref, x_sem.at[2])]
    for copy in small:
        copy.start()

    def move_weights(src, half, move):
        for i in range(n_tile):
            move(wg_hbm.at[src, :, lanes(i)], w1.at[half, i, :, pl.ds(0, LANES)], 0)
            move(wu_hbm.at[src, :, lanes(i)], w1.at[half, i, :, pl.ds(LANES, LANES)], 0)
        for h in range(2):
            for c in range(n_x):
                for k in range(2):
                    move(wd_hbm.at[src, :, lanes((c * 2 + k) * 2 + h)],
                         wd.at[half, h, c, :, pl.ds(k * LANES, LANES)], 1 + h)

    for copy in small:
        copy.wait()
    with jax.named_scope('routing'):
        n_row = slots.shape[0]
        expert = lax.broadcasted_iota(jnp.int32, (n_row, LANES), 0)
        low = lax.broadcasted_iota(jnp.int32, (LANES, LANES), 0)
        high = lax.broadcasted_iota(jnp.int32, (LANES, LANES), 1)
        before = jnp.where(low < high, 1.0, 0.0).astype(BF16)
        ones = jnp.ones((LANES, LANES), BF16)
        delta = lax.rem(expert // 2 - ep + n_ep, n_ep)
        piece = jnp.where(delta == 3, 1, jnp.where(delta == 1, 2, jnp.where(delta == 2, 3, 0)))
        base = (piece * 2 * cap + lax.rem(expert, 2) * unit + 1).astype(F32)
        carry = jnp.zeros((n_row, LANES), F32)
        cols[...] = jnp.zeros_like(cols)
        for b in range(tokens // LANES):
            span = slice(b * LANES, (b + 1) * LANES)
            hit = [expert == ids_ref[j:j + 1, span] for j in range(2)]
            mask = jnp.where(hit[0] | hit[1], 1.0, 0.0)
            rank = jnp.dot(mask.astype(BF16), before, preferred_element_type=F32) + carry
            carry = carry + jnp.dot(mask.astype(BF16), ones, preferred_element_type=F32)
            kept = rank < float(cap)
            slots[:, span] = jnp.where((mask > 0.0) & kept, rank, -1.0)
            where_to = jnp.where(kept, base + rank + jnp.where(rank < float(unit), 0.0, float(unit)), 0.0)
            for j in range(2):
                cols[j:j + 1, span] = jnp.sum(jnp.where(hit[j], where_to, 0.0), axis=0, keepdims=True) - 1.0
                cols[2 + j:3 + j, span] = gates_ref[j:j + 1, span]

    x_copy.wait()
    move_weights(core, 0, lambda src, dst, i: pltpu.make_async_copy(src, dst, w_sem.at[0, i]).start())


    def pick(expert_id, dst):
        with jax.named_scope('pick'):
            row = slots[pl.ds(expert_id, 1), :]
            slot = lax.broadcasted_iota(jnp.int32, (cap, tokens), 0).astype(F32)
            onehot[...] = jnp.where(slot == row, 1.0, 0.0).astype(BF16)
            step = 512
            for c in range(d_model // step):
                got = jnp.dot(onehot[...], xv[:, c * step:(c + 1) * step], preferred_element_type=F32).astype(BF16)
                for u in range(2):
                    dst[u, :, c * step:(c + 1) * step] = got[u * unit:(u + 1) * unit]

    def send_rows(i, u, land, to):
        return remote(xs.at[i, u], xr.at[land], d_send.at[i, u], d_recv.at[land], to, tp)

    quarter = d_model // 4
    parity = lax.rem(xpos, 2)

    def columns(q):
        return pl.ds(pl.multiple_of((2 * parity + q) * quarter, quarter), quarter)

    mine = pl.ds(pl.multiple_of(2 * parity * quarter, 2 * quarter), 2 * quarter)

    def strip(p):
        return pl.ds(p * (unit // 2), unit // 2)

    def send_half(i, land, to, p):
        return remote(xs.at[i, 0, strip(p), mine], xr.at[land, strip(p), mine],
                      h_send.at[i, p], h_recv.at[land - 2, p], to, tp)

    def forward(u, p, q, to):
        at = xr.at[u, strip(p), columns(q)]
        return remote(at, at, f_send.at[u - 2, p, q], f_recv.at[u - 2, p, q], ep, to)

    near = [[send_half(0, 3, yp, 0), send_half(0, 3, yp, 1), send_rows(0, 1, 5, yp)],
            [send_half(1, 2, ym, 0), send_half(1, 2, ym, 1), send_rows(1, 1, 4, ym)]]
    far = [send_rows(2, 0, 6, y2), send_rows(2, 1, 7, y2)]
    pick(2 * yp + core, xs.at[0])
    with jax.named_scope('barrier'):
        pl.semaphore_wait(barrier, len(peers))
    for copy in near[0]:
        copy.start()
    move_weights(other, 1, lambda src, dst, i: remote(src, dst, w_send.at[i], w_sem.at[1, i], ep, partner).start())
    pick(2 * ym + core, xs.at[1])
    for copy in near[1]:
        copy.start()
    pick(2 * ep + core, xr.at[pl.ds(0, 2)])

    def scatter(g, u, n, h, d):
        c = lax.rem(xpos + d, n_x)
        at = pl.ds(u, n)
        return remote(part.at[at, h, c], rv.at[at, h, d - 1], rs_send.at[g, h, d - 1], rs_recv.at[g, h, d - 1],
                      ep, 2 * c + core)

    def total(g, u, n, h):
        with jax.named_scope('wait_rs'):
            for d in range(1, n_x):
                scatter(g, u, n, h, d).wait_recv()
        with jax.named_scope('total'):
            for i in range(n):
                t = part[u + i, h, xpos].astype(F32)
                for d in range(1, n_x):
                    t = t + rv[u + i, h, d - 1].astype(F32)
                t = t.astype(BF16)
                for k in range(2):
                    red[u + i, h, k] = t[:, k * LANES:(k + 1) * LANES]

    back = {2: (yp, 1, 0), 3: (ym, 2, 0), 4: (yp, 1, 1), 5: (ym, 2, 1), 6: (y2, 3, 0), 7: (y2, 3, 1)}

    def returns(u, h):
        to, q, b = back[u]
        return [remote(red.at[u, h, k], ret.at[h, q, b, core], rt_send.at[u, h, k], rt_recv.at[h, q, b, core],
                       to, 2 * xpos + k) for k in range(2)]

    def ffn(g, u, n, first=None, send=True, also=None):
        rows = n * unit
        at = pl.ds(u, n)

        def gate_up(half, _):
            with jax.named_scope('gate_up'):
                for i in range(n_tile):
                    ab = jnp.dot(xr[at].reshape(rows, d_model), w1[half, i], preferred_element_type=F32)
                    a, b = ab[:, :LANES], ab[:, LANES:]
                    hid[half, 0:rows, i * LANES:(i + 1) * LANES] = (jax.nn.silu(a) * b).astype(BF16)
            return 0

        if first is None:
            lax.fori_loop(0, 2, gate_up, 0)
        else:
            for half in range(2):
                with jax.named_scope('wait_w1'):
                    here(w1.at[half], w_sem.at[half, 0])
                gate_up(half, 0)
                if half == 0:
                    first()

        def down(h, _):
            if first:
                with jax.named_scope('wait_wd'):
                    for half in range(2):
                        here(wd.at[half, h], w_sem.at[half, 1 + h])
            with jax.named_scope('down'):
                for c in range(n_x):
                    o = jnp.dot(hid[0, 0:rows], wd[0, h, c], preferred_element_type=F32)
                    o = o + jnp.dot(hid[1, 0:rows], wd[1, h, c], preferred_element_type=F32)
                    part[at, h, c] = o.astype(BF16).reshape(n, unit, 2 * LANES)
                if send:
                    for d in range(1, n_x):
                        scatter(g, u, n, h, d).start()
                if also is not None:
                    @pl.when(also == (h == 1))
                    def _():
                        for d in range(1, n_x):
                            scatter(6, 1, 1, h, d).start()
            return 0

        lax.fori_loop(0, 2, down, 0)

    def return_own(b, h):
        return remote(red.at[b, h, other], ret.at[h, 0, b, core], rt_send.at[b, h, 0], rt_recv.at[h, 0, b, core],
                      ep, partner)

    def keep_own(b, h):
        return_own(b, h).start()
        ret[h, 0, b, core] = red[b, h, core]

    def between():
        pick(2 * y2 + core, xs.at[2])
        for b in range(tokens // LANES):
            colsT[b * LANES:(b + 1) * LANES, :] = cols[:, b * LANES:(b + 1) * LANES].T
        with jax.named_scope('forward'):
            for p in range(2):
                for u in (2, 3):
                    here(xr.at[u, strip(p), mine], h_recv.at[u - 2, p])
                    forward(u, p, 0, right).start()
                    forward(u, p, 1, left).start()

    ffn(0, 0, 1, first=between)

    def near_unit(i, _):
        u = 2 + i
        with jax.named_scope('wait_rows'):
            for p in range(2):
                for q in range(2):
                    here(xr.at[u, strip(p), columns(q)], f_recv.at[i, p, q])
        ffn(1 + i, u, 1)

        @pl.when(i == 0)
        def _():
            with jax.named_scope('near_done'):
                for copy in near[0] + near[1]:
                    copy.wait_send()
                pl.semaphore_signal(both, inc=1, device_id={'ep': ep, 'tp': partner}, device_id_type=MESH)
                pl.semaphore_wait(both, 1)
            for copy in far:
                copy.start()

        @pl.when(i == 1)
        def _():
            for h in range(2):
                total(0, 0, 1, h)
                keep_own(0, h)
        return 0

    lax.fori_loop(0, 2, near_unit, 0)
    with jax.named_scope('wait_rows'):
        for u in (4, 5):
            here(xr.at[u], d_recv.at[u])
    ffn(3, 4, 2)
    ffn(6, 1, 1, send=False)
    for u in (2, 3):
        for h in range(2):
            total(u - 1, u, 1, h)
            for copy in returns(u, h):
                copy.start()

    rows = tokens // 4
    span = 2 * unit

    def choose(at, j, first_slot, n):
        slot = (lax.broadcasted_iota(jnp.int32, (rows, n), 1) + first_slot).astype(F32)
        return jnp.where(colsT[at, j:j + 1] == slot, 1.0, 0.0).astype(BF16)

    def combine(q, b, n, fresh):
        with jax.named_scope('combine'):
            def block(i, _):
                at = pl.ds(pl.multiple_of(i * rows, rows), rows)
                t = jnp.zeros((rows, 2 * LANES), F32) if fresh else acc[at, :]
                y = jnp.concatenate([ret[h, q, pl.ds(b, n)].reshape(n * span, LANES) for h in range(2)], axis=1)
                for j in range(2):
                    got = jnp.dot(choose(at, j, q * 2 * cap + b * span, n * span), y, preferred_element_type=F32)
                    t = t + colsT[at, 2 + j:3 + j] * got
                acc[at, :] = t
                return 0

            lax.fori_loop(0, 4, block, 0)

    def wait_ret(h, q, b):
        with jax.named_scope('wait_ret'):
            for k in range(2):
                here(ret.at[h, q, b, k], rt_recv.at[h, q, b, k])

    def wait_own(h, b):
        with jax.named_scope('wait_own'):
            here(ret.at[h, 0, b, other], rt_recv.at[h, 0, b, other])

    for h in range(2):
        wait_own(h, 0)
    combine(0, 0, 1, True)

    def pick_last(i, _):
        at = pl.ds(pl.multiple_of(i * rows, rows), rows)
        for j in range(2):
            for w, q in enumerate((3, 0)):
                sel[j, at, w * span:(w + 1) * span] = choose(at, j, q * 2 * cap + span, span)
        return 0

    def tail(i, _):
        u = 6 + i
        with jax.named_scope('wait_rows'):
            here(xr.at[u], d_recv.at[u])
        ffn(4 + i, u, 1, also=i == 1)

        @pl.when(i == 0)
        def _():
            lax.fori_loop(0, 4, pick_last, 0)
            for h in range(2):
                total(3, 4, 2, h)
                for w in (4, 5):
                    for copy in returns(w, h):
                        copy.start()
        return 0

    lax.fori_loop(0, 2, tail, 0)

    def combine_near(q):
        for h in range(2):
            for b in range(2):
                wait_ret(h, q, b)
        combine(q, 0, 2, False)

    def last_far(h):
        total(5, 7, 1, h)
        for copy in returns(7, h):
            copy.start()

    def last_own(h):
        total(6, 1, 1, h)
        keep_own(1, h)

    for h in range(2):
        total(4, 6, 1, h)
        for copy in returns(6, h):
            copy.start()
    combine_near(1)
    last_far(0)
    combine_near(2)
    last_own(0)
    last_far(1)
    for h in range(2):
        wait_ret(h, 3, 0)
    combine(3, 0, 1, False)

    half_rows = tokens // 2

    def place(t, h, p):
        at = slice(None) if p is None else pl.ds(p * half_rows, half_rows)
        return out.at[at, pl.ds(pl.multiple_of((2 * t + h) * LANES, LANES), LANES)]

    def spread(t, h, p, to, i):
        return remote(place(t, h, p), place(t, h, p), ag_send.at[h, i], ag_recv.at[h, i], ep, to)

    def publish(t, h, p, i):
        return remote(place(t, h, p), place(t, h, p), p_send.at[h, i], p_recv.at[h, i], ep, partner)

    started = []

    def go(copy):
        copy.start()
        started.append(copy)

    def finish(h):
        wait_own(h, 1)
        wait_ret(h, 3, 1)
        with jax.named_scope('last'):
            y = jnp.concatenate([ret[h, 3, 1].reshape(span, LANES), ret[h, 0, 1].reshape(span, LANES)], axis=0)
            for i in range(4):
                at = slice(i * rows, (i + 1) * rows)
                t = acc[at, h * LANES:(h + 1) * LANES]
                for j in range(2):
                    got = jnp.dot(sel[j, at, :], y, preferred_element_type=F32)
                    t = t + colsT[at, 2 + j:3 + j] * got
                out[at, pl.ds(pl.multiple_of((2 * tp + h) * LANES, LANES), LANES)] = t.astype(BF16)
        go(spread(tp, h, 0, right, 0))
        go(spread(tp, h, 1, left, 3))
        go(spread(tp, h, 1, right, 1))
        go(spread(tp, h, 0, left, 2))
        go(publish(tp, h, None, 0))

    def relay(h):
        with jax.named_scope('relay'):
            spread(left, h, 0, right, 0).wait_recv()
            go(spread(left, h, 0, right, 4))
            spread(right, h, 1, left, 3).wait_recv()
            go(spread(right, h, 1, left, 5))
            go(publish(left, h, 0, 1))
            go(publish(right, h, 1, 2))

    finish(0)
    last_own(1)
    finish(1)
    relay(0)
    relay(1)
    with jax.named_scope('gather'):
        for h in range(2):
            spread(left, h, 1, right, 1).wait_recv()
            go(publish(left, h, 1, 3))
            spread(right, h, 0, left, 2).wait_recv()
            go(publish(right, h, 0, 4))
        for h in range(2):
            spread(across, h, 0, right, 4).wait_recv()
            go(publish(across, h, 0, 5))
            spread(across, h, 1, left, 5).wait_recv()
            go(publish(across, h, 1, 6))
        for h in range(2):
            for i in range(7):
                publish(tp, h, None if i == 0 else 0, i).wait_recv()

    with jax.named_scope('drain'):
        for copy in far + started:
            copy.wait_send()
        here(w1.at[1], w_send.at[0])
        for u in (2, 3):
            for p in range(2):
                forward(u, p, 0, right).wait_send()
                forward(u, p, 1, left).wait_send()
        for h in range(2):
            here(wd.at[1, h], w_send.at[1 + h])
        for h in range(2):
            for b in range(2):
                return_own(b, h).wait_send()
            for u in back:
                for copy in returns(u, h):
                    copy.wait_send()
            for d in range(1, n_x):
                for g, u, n in ((0, 0, 1), (1, 2, 1), (2, 3, 1), (3, 4, 2), (4, 6, 1), (5, 7, 1), (6, 1, 1)):
                    scatter(g, u, n, h, d).wait_send()


def solution(mesh):
    n_ep = mesh.shape['ep']
    n_tp = mesh.shape['tp']
    row_spec = P(('dp', 'ep'), None)

    def device_body(x_loc, ids_loc, gates_loc, wg_loc, wu_loc, wd_loc):
        tokens, d_model = x_loc.shape
        n_top = ids_loc.shape[1]
        local_experts, _, ff = wg_loc.shape
        n_experts = local_experts * n_ep
        cap = CAP_NUM * n_top * tokens // (CAP_DEN * n_experts)
        unit = cap // 2
        n_x = n_tp // 2
        n_tile = ff // LANES
        vmem = pltpu.VMEM
        dma = pltpu.SemaphoreType.DMA

        def kernel(*refs):
            moe_kernel(n_ep, n_tp, cap, *refs)

        any_spec = pl.BlockSpec(memory_space=pl.ANY)
        vmem_spec = pl.BlockSpec(memory_space=pltpu.VMEM)
        return pl.pallas_call(
            kernel,
            out_shape=pltpu.VMEM((tokens, d_model), BF16),
            in_specs=[any_spec] * 6,
            out_specs=vmem_spec,
            scratch_shapes=[
                vmem(ids_loc.shape[::-1], jnp.int32),
                vmem(gates_loc.shape[::-1], F32),
                vmem((tokens, d_model), BF16),
                vmem((cap, tokens), BF16),
                vmem((3, 2, unit, d_model), BF16),
                vmem((8, unit, d_model), BF16),
                vmem((2, n_tile, d_model, 2 * LANES), BF16),
                vmem((2, 2, n_x, ff, 2 * LANES), BF16),
                vmem((2, cap, ff), BF16),
                vmem((8, 2, n_x, unit, 2 * LANES), BF16),
                vmem((8, 2, n_x - 1, unit, 2 * LANES), BF16),
                vmem((8, 2, 2, unit, LANES), BF16),
                vmem((2, 4, 2, 2, unit, LANES), BF16),
                vmem((tokens, 2 * LANES), F32),
                vmem((2 * n_experts, tokens), F32),
                vmem((LANES, tokens), F32),
                vmem((tokens, LANES), F32),
                vmem((2, tokens, 4 * unit), BF16),
                dma((3,)), dma((2, 3)), dma((3,)), dma((3, 2)), dma((8,)),
                dma((7, 2, n_x - 1)), dma((7, 2, n_x - 1)), dma((8, 2, 2)), dma((2, 4, 2, 2)),
                dma((2, 6)), dma((2, 6)), dma((2, 7)), dma((2, 7)), dma((2, 2, 2)), dma((2, 2, 2)), dma((2, 2)), dma((2, 2)),
                pltpu.SemaphoreType.REGULAR,
            ],
            compiler_params=pltpu.CompilerParams(
                collective_id=0, has_side_effects=True, vmem_limit_bytes=58 * 1024 * 1024),
        )(ids_loc.T, gates_loc.T, x_loc, wg_loc, wu_loc, wd_loc)

    return jax.shard_map(device_body, mesh=mesh,
                         in_specs=(row_spec, row_spec, row_spec, P('ep', None, 'tp'), P('ep', None, 'tp'), P('ep', 'tp', None)),
                         out_specs=row_spec, check_vma=False)
```

```python
import jax
import jax.numpy as jnp
from jax import lax
from jax.experimental import pallas as pl
from jax.experimental.pallas import tpu as pltpu
from jax.sharding import PartitionSpec as P

CAP_NUM = 5
CAP_DEN = 4
LANES = 128
MESH = pl.DeviceIdType.MESH
BF16 = jnp.bfloat16
F32 = jnp.float32


def moe_kernel(n_ep, n_tp, cap,
               ids_hbm, gates_hbm, x_hbm, wg_hbm, wu_hbm, wd_hbm, out,
               ids_ref, gates_ref, xv, onehot, xs, xr, w1, wd, hid, part, rv, red, ret, acc, slots, cols, colsT, sel,
               x_sem, w_sem, w_send, d_send, d_recv, rs_send, rs_recv, rt_send, rt_recv,
               ag_send, ag_recv, p_send, p_recv, f_send, f_recv, h_recv, both):
    tokens, d_model = x_hbm.shape
    n_x = n_tp // 2
    n_tile = w1.shape[1]
    unit = cap // 2
    ep = lax.axis_index('ep')
    tp = lax.axis_index('tp')
    core = lax.rem(tp, 2)
    other = 1 - core
    xpos = tp // 2
    partner = tp + 1 - 2 * core
    yp, y2, ym = [lax.rem(ep + i, n_ep) for i in (1, 2, 3)]
    right, left = lax.rem(tp + 2, n_tp), lax.rem(tp + n_tp - 2, n_tp)
    across = lax.rem(tp + 4, n_tp)

    def remote(src, dst, ss, rs, ep_to, tp_to):
        return pltpu.make_async_remote_copy(src_ref=src, dst_ref=dst, send_sem=ss, recv_sem=rs,
                                            device_id={'ep': ep_to, 'tp': tp_to}, device_id_type=MESH)

    def here(ref, sem):
        pltpu.make_async_copy(ref, ref, sem).wait()

    def lanes(i):
        return pl.ds(i * LANES, LANES)

    barrier = pltpu.get_barrier_semaphore()
    peers = [(ep, partner)] + [(e, t) for e in (yp, ym, y2) for t in (tp, partner)]
    peers += [(ep, t) for t in (right, across, left)]
    for e, t in peers:
        pl.semaphore_signal(barrier, inc=1, device_id={'ep': e, 'tp': t}, device_id_type=MESH)

    x_copy = pltpu.make_async_copy(x_hbm, xv, x_sem.at[0])
    x_copy.start()
    small = [pltpu.make_async_copy(ids_hbm, ids_ref, x_sem.at[1]), pltpu.make_async_copy(gates_hbm, gates_ref, x_sem.at[2])]
    for copy in small:
        copy.start()

    def move_weights(src, half, move):
        for i in range(n_tile):
            move(wg_hbm.at[src, :, lanes(i)], w1.at[half, i, :, pl.ds(0, LANES)], 0)
            move(wu_hbm.at[src, :, lanes(i)], w1.at[half, i, :, pl.ds(LANES, LANES)], 0)
        for h in range(2):
            for c in range(n_x):
                for k in range(2):
                    move(wd_hbm.at[src, :, lanes((c * 2 + k) * 2 + h)],
                         wd.at[half, h, c, :, pl.ds(k * LANES, LANES)], 1 + h)

    for copy in small:
        copy.wait()
    with jax.named_scope('routing'):
        n_row = slots.shape[0]
        expert = lax.broadcasted_iota(jnp.int32, (n_row, LANES), 0)
        low = lax.broadcasted_iota(jnp.int32, (LANES, LANES), 0)
        high = lax.broadcasted_iota(jnp.int32, (LANES, LANES), 1)
        before = jnp.where(low < high, 1.0, 0.0).astype(BF16)
        ones = jnp.ones((LANES, LANES), BF16)
        delta = lax.rem(expert // 2 - ep + n_ep, n_ep)
        piece = jnp.where(delta == 3, 1, jnp.where(delta == 1, 2, jnp.where(delta == 2, 3, 0)))
        base = (piece * 2 * cap + lax.rem(expert, 2) * unit + 1).astype(F32)
        carry = jnp.zeros((n_row, LANES), F32)
        cols[...] = jnp.zeros_like(cols)
        for b in range(tokens // LANES):
            span = slice(b * LANES, (b + 1) * LANES)
            hit = [expert == ids_ref[j:j + 1, span] for j in range(2)]
            mask = jnp.where(hit[0] | hit[1], 1.0, 0.0)
            rank = jnp.dot(mask.astype(BF16), before, preferred_element_type=F32) + carry
            carry = carry + jnp.dot(mask.astype(BF16), ones, preferred_element_type=F32)
            kept = rank < float(cap)
            slots[:, span] = jnp.where((mask > 0.0) & kept, rank, -1.0)
            where_to = jnp.where(kept, base + rank + jnp.where(rank < float(unit), 0.0, float(unit)), 0.0)
            for j in range(2):
                cols[j:j + 1, span] = jnp.sum(jnp.where(hit[j], where_to, 0.0), axis=0, keepdims=True) - 1.0
                cols[2 + j:3 + j, span] = gates_ref[j:j + 1, span]

    x_copy.wait()
    move_weights(core, 0, lambda src, dst, i: pltpu.make_async_copy(src, dst, w_sem.at[0, i]).start())


    def pick(expert_id, dst):
        with jax.named_scope('pick'):
            row = slots[pl.ds(expert_id, 1), :]
            slot = lax.broadcasted_iota(jnp.int32, (cap, tokens), 0).astype(F32)
            onehot[...] = jnp.where(slot == row, 1.0, 0.0).astype(BF16)
            step = 512
            for c in range(d_model // step):
                got = jnp.dot(onehot[...], xv[:, c * step:(c + 1) * step], preferred_element_type=F32).astype(BF16)
                for u in range(2):
                    dst[u, :, c * step:(c + 1) * step] = got[u * unit:(u + 1) * unit]

    quarter = d_model // 4
    parity = lax.rem(xpos, 2)

    def columns(q):
        return pl.ds(pl.multiple_of((2 * parity + q) * quarter, quarter), quarter)

    mine = pl.ds(pl.multiple_of(2 * parity * quarter, 2 * quarter), 2 * quarter)

    def strip(p):
        return pl.ds(p * (unit // 2), unit // 2)

    def send_half(i, land, to, p):
        return remote(xs.at[i, 0, strip(p), mine], xr.at[land, strip(p), mine],
                      d_send.at[0], h_recv.at[p], to, tp)

    def send_near(i, land, to):
        return remote(xs.at[i, 1], xr.at[land], d_send.at[0], d_recv.at[0], to, tp)

    def send_far(u):
        return remote(xs.at[2, u], xr.at[6 + u], d_send.at[1], d_recv.at[1 + u], y2, tp)

    def forward(u, p, q, to):
        at = xr.at[u, strip(p), columns(q)]
        return remote(at, at, f_send.at[0], f_recv.at[u - 2], ep, to)

    near = [[send_half(0, 3, yp, 0), send_half(0, 3, yp, 1), send_near(0, 5, yp)],
            [send_half(1, 2, ym, 0), send_half(1, 2, ym, 1), send_near(1, 4, ym)]]
    far = [send_far(0), send_far(1)]
    pick(2 * yp + core, xs.at[0])
    with jax.named_scope('barrier'):
        pl.semaphore_wait(barrier, len(peers))
    for copy in near[0]:
        copy.start()
    move_weights(other, 1, lambda src, dst, i: remote(src, dst, w_send.at[min(i, 1)], w_sem.at[1, i], ep, partner).start())
    pick(2 * ym + core, xs.at[1])
    for copy in near[1]:
        copy.start()
    pick(2 * ep + core, xr.at[pl.ds(0, 2)])

    def scatter(g, u, n, h, d):
        c = lax.rem(xpos + d, n_x)
        at = pl.ds(u, n)
        return remote(part.at[at, h, c], rv.at[at, h, d - 1], rs_send.at[0], rs_recv.at[g, h],
                      ep, 2 * c + core)

    def total(g, u, n, h):
        with jax.named_scope('wait_rs'):
            here(rv.at[pl.ds(u, n), h], rs_recv.at[g, h])
        with jax.named_scope('total'):
            for i in range(n):
                t = part[u + i, h, xpos].astype(F32)
                for d in range(1, n_x):
                    t = t + rv[u + i, h, d - 1].astype(F32)
                t = t.astype(BF16)
                for k in range(2):
                    red[u + i, h, k] = t[:, k * LANES:(k + 1) * LANES]

    back = {2: (yp, 1, 0), 3: (ym, 2, 0), 4: (yp, 1, 1), 5: (ym, 2, 1), 6: (y2, 3, 0), 7: (y2, 3, 1)}

    def returns(u, h):
        to, q, b = back[u]
        sem = q - 1 if q < 3 else 2 + b * (1 + h)
        return [remote(red.at[u, h, k], ret.at[h, q, b, core], rt_send.at[0], rt_recv.at[sem],
                       to, 2 * xpos + k) for k in range(2)]

    def ffn(g, u, n, first=None, send=True, also=None):
        rows = n * unit
        at = pl.ds(u, n)

        def gate_up(half, _):
            with jax.named_scope('gate_up'):
                for i in range(n_tile):
                    ab = jnp.dot(xr[at].reshape(rows, d_model), w1[half, i], preferred_element_type=F32)
                    a, b = ab[:, :LANES], ab[:, LANES:]
                    hid[half, 0:rows, i * LANES:(i + 1) * LANES] = (jax.nn.silu(a) * b).astype(BF16)
            return 0

        if first is None:
            lax.fori_loop(0, 2, gate_up, 0)
        else:
            for half in range(2):
                with jax.named_scope('wait_w1'):
                    here(w1.at[half], w_sem.at[half, 0])
                gate_up(half, 0)
                if half == 0:
                    first()

        def down(h, _):
            if first:
                with jax.named_scope('wait_wd'):
                    for half in range(2):
                        here(wd.at[half, h], w_sem.at[half, 1 + h])
            with jax.named_scope('down'):
                for c in range(n_x):
                    o = jnp.dot(hid[0, 0:rows], wd[0, h, c], preferred_element_type=F32)
                    o = o + jnp.dot(hid[1, 0:rows], wd[1, h, c], preferred_element_type=F32)
                    part[at, h, c] = o.astype(BF16).reshape(n, unit, 2 * LANES)
                if send:
                    for d in range(1, n_x):
                        scatter(g, u, n, h, d).start()
                if also is not None:
                    @pl.when(also == (h == 1))
                    def _():
                        for d in range(1, n_x):
                            scatter(6, 1, 1, h, d).start()
            return 0

        lax.fori_loop(0, 2, down, 0)

    def return_own(b, h):
        return remote(red.at[b, h, other], ret.at[h, 0, b, core], rt_send.at[0], rt_recv.at[5 + b * (1 + h)],
                      ep, partner)

    def keep_own(b, h):
        return_own(b, h).start()
        ret[h, 0, b, core] = red[b, h, core]

    def between():
        pick(2 * y2 + core, xs.at[2])
        for b in range(tokens // LANES):
            colsT[b * LANES:(b + 1) * LANES, :] = cols[:, b * LANES:(b + 1) * LANES].T
        with jax.named_scope('forward'):
            for p in range(2):
                here(xr.at[pl.ds(2, 2), strip(p), mine], h_recv.at[p])
                for u in (2, 3):
                    forward(u, p, 0, right).start()
                    forward(u, p, 1, left).start()

    ffn(0, 0, 1, first=between)

    def near_unit(i, _):
        u = 2 + i
        with jax.named_scope('wait_rows'):
            theirs = pl.ds(pl.multiple_of(2 * (1 - parity) * quarter, 2 * quarter), 2 * quarter)
            here(xr.at[u, :, theirs], f_recv.at[i])
        ffn(1 + i, u, 1)

        @pl.when(i == 0)
        def _():
            with jax.named_scope('near_done'):
                here(xr.at[pl.ds(0, 3)], d_send.at[0])
                pl.semaphore_signal(both, inc=1, device_id={'ep': ep, 'tp': partner}, device_id_type=MESH)
                pl.semaphore_wait(both, 1)
            for copy in far:
                copy.start()

        @pl.when(i == 1)
        def _():
            for h in range(2):
                total(0, 0, 1, h)
                keep_own(0, h)
        return 0

    lax.fori_loop(0, 2, near_unit, 0)
    with jax.named_scope('wait_rows'):
        here(xr.at[pl.ds(4, 2)], d_recv.at[0])
    ffn(3, 4, 2)
    ffn(6, 1, 1, send=False)
    for u in (2, 3):
        for h in range(2):
            total(u - 1, u, 1, h)
            for copy in returns(u, h):
                copy.start()

    rows = tokens // 4
    span = 2 * unit

    def choose(at, j, first_slot, n):
        slot = (lax.broadcasted_iota(jnp.int32, (rows, n), 1) + first_slot).astype(F32)
        return jnp.where(colsT[at, j:j + 1] == slot, 1.0, 0.0).astype(BF16)

    def combine(q, b, n, fresh):
        with jax.named_scope('combine'):
            def block(i, _):
                at = pl.ds(pl.multiple_of(i * rows, rows), rows)
                t = jnp.zeros((rows, 2 * LANES), F32) if fresh else acc[at, :]
                y = jnp.concatenate([ret[h, q, pl.ds(b, n)].reshape(n * span, LANES) for h in range(2)], axis=1)
                for j in range(2):
                    got = jnp.dot(choose(at, j, q * 2 * cap + b * span, n * span), y, preferred_element_type=F32)
                    t = t + colsT[at, 2 + j:3 + j] * got
                acc[at, :] = t
                return 0

            lax.fori_loop(0, 4, block, 0)

    def wait_ret(ref, i):
        with jax.named_scope('wait_ret'):
            here(ref, rt_recv.at[i])

    wait_ret(ret.at[:, 0, 0, other], 5)
    combine(0, 0, 1, True)

    def pick_last(i, _):
        at = pl.ds(pl.multiple_of(i * rows, rows), rows)
        for j in range(2):
            for w, q in enumerate((3, 0)):
                sel[j, at, w * span:(w + 1) * span] = choose(at, j, q * 2 * cap + span, span)
        return 0

    def tail(i, _):
        u = 6 + i
        with jax.named_scope('wait_rows'):
            here(xr.at[u], d_recv.at[1 + i])
        ffn(4 + i, u, 1, also=i == 1)

        @pl.when(i == 0)
        def _():
            lax.fori_loop(0, 4, pick_last, 0)
            for h in range(2):
                total(3, 4, 2, h)
                for w in (4, 5):
                    for copy in returns(w, h):
                        copy.start()
        return 0

    lax.fori_loop(0, 2, tail, 0)

    def combine_near(q):
        wait_ret(ret.at[:, q], q - 1)
        combine(q, 0, 2, False)

    def last_far(h):
        total(5, 7, 1, h)
        for copy in returns(7, h):
            copy.start()

    def last_own(h):
        total(6, 1, 1, h)
        keep_own(1, h)

    for h in range(2):
        total(4, 6, 1, h)
        for copy in returns(6, h):
            copy.start()
    combine_near(1)
    last_far(0)
    combine_near(2)
    last_own(0)
    last_far(1)
    wait_ret(ret.at[:, 3, 0], 2)
    combine(3, 0, 1, False)

    half_rows = tokens // 2

    def place(t, h, p):
        at = slice(None) if p is None else pl.ds(p * half_rows, half_rows)
        return out.at[at, pl.ds(pl.multiple_of((2 * t + h) * LANES, LANES), LANES)]

    def spread(t, h, p, to, i):
        return remote(place(t, h, p), place(t, h, p), ag_send.at[0], ag_recv.at[h, i], ep, to)

    def publish(t, h, p):
        return remote(place(t, h, p), place(t, h, p), p_send.at[0], p_recv.at[0], ep, partner)

    def go(copy):
        copy.start()

    def finish(h):
        wait_ret(ret.at[h, 0, 1, other], 6 + h)
        wait_ret(ret.at[h, 3, 1], 3 + h)
        with jax.named_scope('last'):
            y = jnp.concatenate([ret[h, 3, 1].reshape(span, LANES), ret[h, 0, 1].reshape(span, LANES)], axis=0)
            for i in range(4):
                at = slice(i * rows, (i + 1) * rows)
                t = acc[at, h * LANES:(h + 1) * LANES]
                for j in range(2):
                    got = jnp.dot(sel[j, at, :], y, preferred_element_type=F32)
                    t = t + colsT[at, 2 + j:3 + j] * got
                out[at, pl.ds(pl.multiple_of((2 * tp + h) * LANES, LANES), LANES)] = t.astype(BF16)
        go(spread(tp, h, 0, right, 0))
        go(spread(tp, h, 1, left, 3))
        go(spread(tp, h, 1, right, 1))
        go(spread(tp, h, 0, left, 2))
        go(publish(tp, h, None))

    def relay(h):
        with jax.named_scope('relay'):
            spread(left, h, 0, right, 0).wait_recv()
            go(spread(left, h, 0, right, 4))
            spread(right, h, 1, left, 3).wait_recv()
            go(spread(right, h, 1, left, 5))
            go(publish(left, h, 0))
            go(publish(right, h, 1))

    finish(0)
    last_own(1)
    finish(1)
    relay(0)
    relay(1)
    with jax.named_scope('gather'):
        for h in range(2):
            spread(left, h, 1, right, 1).wait_recv()
            go(publish(left, h, 1))
            spread(right, h, 0, left, 2).wait_recv()
            go(publish(right, h, 0))
        for h in range(2):
            spread(across, h, 0, right, 4).wait_recv()
            go(publish(across, h, 0))
            spread(across, h, 1, left, 5).wait_recv()
            go(publish(across, h, 1))
        here(out.at[:, pl.ds(0, 8 * LANES)], p_recv.at[0])

    with jax.named_scope('drain'):
        here(xs.at[2], d_send.at[1])
        here(w1.at[1], w_send.at[0])
        here(wd.at[1], w_send.at[1])
        here(xr.at[0], f_send.at[0])
        here(rv, rs_send.at[0])
        here(red.at[pl.ds(0, 7)], rt_send.at[0])
        here(out.at[:, pl.ds(0, 6 * LANES)], ag_send.at[0])
        here(out.at[:, pl.ds(0, 8 * LANES)], p_send.at[0])


def solution(mesh):
    n_ep = mesh.shape['ep']
    n_tp = mesh.shape['tp']
    row_spec = P(('dp', 'ep'), None)

    def device_body(x_loc, ids_loc, gates_loc, wg_loc, wu_loc, wd_loc):
        tokens, d_model = x_loc.shape
        n_top = ids_loc.shape[1]
        local_experts, _, ff = wg_loc.shape
        n_experts = local_experts * n_ep
        cap = CAP_NUM * n_top * tokens // (CAP_DEN * n_experts)
        unit = cap // 2
        n_x = n_tp // 2
        n_tile = ff // LANES
        vmem = pltpu.VMEM
        dma = pltpu.SemaphoreType.DMA

        def kernel(*refs):
            moe_kernel(n_ep, n_tp, cap, *refs)

        any_spec = pl.BlockSpec(memory_space=pl.ANY)
        vmem_spec = pl.BlockSpec(memory_space=pltpu.VMEM)
        return pl.pallas_call(
            kernel,
            out_shape=pltpu.VMEM((tokens, d_model), BF16),
            in_specs=[any_spec] * 6,
            out_specs=vmem_spec,
            scratch_shapes=[
                vmem(ids_loc.shape[::-1], jnp.int32),
                vmem(gates_loc.shape[::-1], F32),
                vmem((tokens, d_model), BF16),
                vmem((cap, tokens), BF16),
                vmem((3, 2, unit, d_model), BF16),
                vmem((8, unit, d_model), BF16),
                vmem((2, n_tile, d_model, 2 * LANES), BF16),
                vmem((2, 2, n_x, ff, 2 * LANES), BF16),
                vmem((2, cap, ff), BF16),
                vmem((8, 2, n_x, unit, 2 * LANES), BF16),
                vmem((8, 2, n_x - 1, unit, 2 * LANES), BF16),
                vmem((8, 2, 2, unit, LANES), BF16),
                vmem((2, 4, 2, 2, unit, LANES), BF16),
                vmem((tokens, 2 * LANES), F32),
                vmem((2 * n_experts, tokens), F32),
                vmem((LANES, tokens), F32),
                vmem((tokens, LANES), F32),
                vmem((2, tokens, 4 * unit), BF16),
                dma((3,)), dma((2, 3)), dma((2,)), dma((2,)), dma((3,)),
                dma((1,)), dma((7, 2)), dma((1,)), dma((8,)),
                dma((1,)), dma((2, 6)), dma((1,)), dma((1,)), dma((1,)), dma((2,)), dma((2,)),
                pltpu.SemaphoreType.REGULAR,
            ],
            compiler_params=pltpu.CompilerParams(
                collective_id=0, has_side_effects=True, vmem_limit_bytes=58 * 1024 * 1024),
        )(ids_loc.T, gates_loc.T, x_loc, wg_loc, wu_loc, wd_loc)

    return jax.shard_map(device_body, mesh=mesh,
                         in_specs=(row_spec, row_spec, row_spec, P('ep', None, 'tp'), P('ep', None, 'tp'), P('ep', 'tp', None)),
                         out_specs=row_spec, check_vma=False)
```

```python
import jax
import jax.numpy as jnp
from jax import lax
from jax.experimental import pallas as pl
from jax.experimental.pallas import tpu as pltpu
from jax.sharding import PartitionSpec as P

CAP_NUM = 5
CAP_DEN = 4
LANES = 128
MESH = pl.DeviceIdType.MESH
BF16 = jnp.bfloat16
F32 = jnp.float32


def moe_kernel(n_ep, n_tp, cap,
               ids_hbm, gates_hbm, x_hbm, wg_hbm, wu_hbm, wd_hbm, out,
               ids_ref, gates_ref, xv, onehot, xs, xr, w1, wd, hid, part, rv, red, ret, acc, slots, cols, colsT, sel,
               x_sem, w_sem, w_send, d_send, d_recv, rs_send, rs_recv, rt_send, rt_recv,
               ag_send, ag_recv, p_send, p_recv, f_send, f_recv, h_recv, both):
    tokens, d_model = x_hbm.shape
    n_x = n_tp // 2
    n_tile = w1.shape[1]
    unit = cap // 2
    ep = lax.axis_index('ep')
    tp = lax.axis_index('tp')
    core = lax.rem(tp, 2)
    other = 1 - core
    xpos = tp // 2
    partner = tp + 1 - 2 * core
    yp, y2, ym = [lax.rem(ep + i, n_ep) for i in (1, 2, 3)]
    right, left = lax.rem(tp + 2, n_tp), lax.rem(tp + n_tp - 2, n_tp)
    across = lax.rem(tp + 4, n_tp)

    def remote(src, dst, ss, rs, ep_to, tp_to):
        return pltpu.make_async_remote_copy(src_ref=src, dst_ref=dst, send_sem=ss, recv_sem=rs,
                                            device_id={'ep': ep_to, 'tp': tp_to}, device_id_type=MESH)

    def here(ref, sem):
        pltpu.make_async_copy(ref, ref, sem).wait()

    def lanes(i):
        return pl.ds(i * LANES, LANES)

    barrier = pltpu.get_barrier_semaphore()
    peers = [(ep, partner)] + [(e, t) for e in (yp, ym, y2) for t in (tp, partner)]
    peers += [(ep, t) for t in (right, across, left)]
    for e, t in peers:
        pl.semaphore_signal(barrier, inc=1, device_id={'ep': e, 'tp': t}, device_id_type=MESH)

    x_copy = pltpu.make_async_copy(x_hbm, xv, x_sem.at[0])
    x_copy.start()
    small = [pltpu.make_async_copy(ids_hbm, ids_ref, x_sem.at[1]), pltpu.make_async_copy(gates_hbm, gates_ref, x_sem.at[2])]
    for copy in small:
        copy.start()

    def move_weights(src, half, move):
        for i in range(n_tile):
            move(wg_hbm.at[src, :, lanes(i)], w1.at[half, i, :, pl.ds(0, LANES)], 0)
            move(wu_hbm.at[src, :, lanes(i)], w1.at[half, i, :, pl.ds(LANES, LANES)], 0)
        for h in range(2):
            for c in range(n_x):
                for k in range(2):
                    move(wd_hbm.at[src, :, lanes((c * 2 + k) * 2 + h)],
                         wd.at[half, h, c, :, pl.ds(k * LANES, LANES)], 1 + h)

    for copy in small:
        copy.wait()
    with jax.named_scope('routing'):
        n_row = slots.shape[0]
        expert = lax.broadcasted_iota(jnp.int32, (n_row, LANES), 0)
        low = lax.broadcasted_iota(jnp.int32, (LANES, LANES), 0)
        high = lax.broadcasted_iota(jnp.int32, (LANES, LANES), 1)
        before = jnp.where(low < high, 1.0, 0.0).astype(BF16)
        ones = jnp.ones((LANES, LANES), BF16)
        delta = lax.rem(expert // 2 - ep + n_ep, n_ep)
        piece = jnp.where(delta == 3, 1, jnp.where(delta == 1, 2, jnp.where(delta == 2, 3, 0)))
        base = (piece * 2 * cap + lax.rem(expert, 2) * unit + 1).astype(F32)
        carry = jnp.zeros((n_row, LANES), F32)
        cols[...] = jnp.zeros_like(cols)
        for b in range(tokens // LANES):
            span = slice(b * LANES, (b + 1) * LANES)
            hit = [expert == ids_ref[j:j + 1, span] for j in range(2)]
            mask = jnp.where(hit[0] | hit[1], 1.0, 0.0)
            rank = jnp.dot(mask.astype(BF16), before, preferred_element_type=F32) + carry
            carry = carry + jnp.dot(mask.astype(BF16), ones, preferred_element_type=F32)
            kept = rank < float(cap)
            slots[:, span] = jnp.where((mask > 0.0) & kept, rank, -1.0)
            where_to = jnp.where(kept, base + rank + jnp.where(rank < float(unit), 0.0, float(unit)), 0.0)
            for j in range(2):
                cols[j:j + 1, span] = jnp.sum(jnp.where(hit[j], where_to, 0.0), axis=0, keepdims=True) - 1.0
                cols[2 + j:3 + j, span] = gates_ref[j:j + 1, span]

    x_copy.wait()
    move_weights(core, 0, lambda src, dst, i: pltpu.make_async_copy(src, dst, w_sem.at[0, i]).start())


    def pick(expert_id, dst):
        with jax.named_scope('pick'):
            row = slots[pl.ds(expert_id, 1), :]
            slot = lax.broadcasted_iota(jnp.int32, (cap, tokens), 0).astype(F32)
            onehot[...] = jnp.where(slot == row, 1.0, 0.0).astype(BF16)
            step = 512
            for c in range(d_model // step):
                got = jnp.dot(onehot[...], xv[:, c * step:(c + 1) * step], preferred_element_type=F32).astype(BF16)
                for u in range(2):
                    dst[u, :, c * step:(c + 1) * step] = got[u * unit:(u + 1) * unit]

    quarter = d_model // 4
    parity = lax.rem(xpos, 2)

    def columns(q):
        return pl.ds(pl.multiple_of((2 * parity + q) * quarter, quarter), quarter)

    mine = pl.ds(pl.multiple_of(2 * parity * quarter, 2 * quarter), 2 * quarter)

    def strip(p):
        return pl.ds(p * (unit // 2), unit // 2)

    def send_half(i, land, to, p):
        return remote(xs.at[i, 0, strip(p), mine], xr.at[land, strip(p), mine],
                      d_send.at[0], h_recv.at[p], to, tp)

    def send_near(i, land, to):
        return remote(xs.at[i, 1], xr.at[land], d_send.at[0], d_recv.at[0], to, tp)

    def send_far(u):
        return remote(xs.at[2, u], xr.at[6 + u], d_send.at[1], d_recv.at[1 + u], y2, tp)

    def forward(u, p, q, to):
        at = xr.at[u, strip(p), columns(q)]
        return remote(at, at, f_send.at[0], f_recv.at[u - 2], ep, to)

    near = [[send_half(0, 3, yp, 0), send_half(0, 3, yp, 1), send_near(0, 5, yp)],
            [send_half(1, 2, ym, 0), send_half(1, 2, ym, 1), send_near(1, 4, ym)]]
    far = [send_far(0), send_far(1)]
    pick(2 * yp + core, xs.at[0])
    with jax.named_scope('barrier'):
        pl.semaphore_wait(barrier, len(peers))
    for copy in near[0]:
        copy.start()
    move_weights(other, 1, lambda src, dst, i: remote(src, dst, w_send.at[min(i, 1)], w_sem.at[1, i], ep, partner).start())
    pick(2 * ym + core, xs.at[1])
    for copy in near[1]:
        copy.start()
    pick(2 * ep + core, xr.at[pl.ds(0, 2)])

    def scatter(g, u, n, h, d):
        c = lax.rem(xpos + d, n_x)
        at = pl.ds(u, n)
        return remote(part.at[at, h, c], rv.at[at, h, d - 1], rs_send.at[0], rs_recv.at[g, h],
                      ep, 2 * c + core)

    def total(g, u, n, h):
        with jax.named_scope('wait_rs'):
            here(rv.at[pl.ds(u, n), h], rs_recv.at[g, h])
        with jax.named_scope('total'):
            for i in range(n):
                t = part[u + i, h, xpos].astype(F32)
                for d in range(1, n_x):
                    t = t + rv[u + i, h, d - 1].astype(F32)
                t = t.astype(BF16)
                for k in range(2):
                    red[u + i, h, k] = t[:, k * LANES:(k + 1) * LANES]

    back = {2: (yp, 1, 0), 3: (ym, 2, 0), 4: (yp, 1, 1), 5: (ym, 2, 1), 6: (y2, 3, 0), 7: (y2, 3, 1)}

    def returns(u, h):
        to, q, b = back[u]
        sem = q - 1 if q < 3 else 2 + b * (1 + h)
        return [remote(red.at[u, h, k], ret.at[h, q, b, core], rt_send.at[0], rt_recv.at[sem],
                       to, 2 * xpos + k) for k in range(2)]

    def ffn(g, u, n, first=None, send=True, also=None):
        rows = n * unit
        at = pl.ds(u, n)

        def gate_up(half, _):
            with jax.named_scope('gate_up'):
                for i in range(n_tile):
                    ab = jnp.dot(xr[at].reshape(rows, d_model), w1[half, i], preferred_element_type=F32)
                    a, b = ab[:, :LANES], ab[:, LANES:]
                    hid[half, 0:rows, i * LANES:(i + 1) * LANES] = (jax.nn.silu(a) * b).astype(BF16)
            return 0

        if first is None:
            lax.fori_loop(0, 2, gate_up, 0)
        else:
            for half in range(2):
                with jax.named_scope('wait_w1'):
                    here(w1.at[half], w_sem.at[half, 0])
                gate_up(half, 0)
                if half == 0:
                    first()

        def down(h, _):
            if first:
                with jax.named_scope('wait_wd'):
                    for half in range(2):
                        here(wd.at[half, h], w_sem.at[half, 1 + h])
            with jax.named_scope('down'):
                for c in range(n_x):
                    o = jnp.dot(hid[0, 0:rows], wd[0, h, c], preferred_element_type=F32)
                    o = o + jnp.dot(hid[1, 0:rows], wd[1, h, c], preferred_element_type=F32)
                    part[at, h, c] = o.astype(BF16).reshape(n, unit, 2 * LANES)
                if send:
                    for d in range(1, n_x):
                        scatter(g, u, n, h, d).start()
                if also is not None:
                    @pl.when(also == (h == 1))
                    def _():
                        for d in range(1, n_x):
                            scatter(6, 1, 1, h, d).start()
            return 0

        lax.fori_loop(0, 2, down, 0)

    def return_own(b, h):
        return remote(red.at[b, h, other], ret.at[h, 0, b, core], rt_send.at[0], rt_recv.at[5 + b * (1 + h)],
                      ep, partner)

    def keep_own(b, h):
        return_own(b, h).start()
        ret[h, 0, b, core] = red[b, h, core]

    def between():
        pick(2 * y2 + core, xs.at[2])
        for b in range(tokens // LANES):
            colsT[b * LANES:(b + 1) * LANES, :] = cols[:, b * LANES:(b + 1) * LANES].T
        with jax.named_scope('forward'):
            for p in range(2):
                here(xr.at[pl.ds(2, 2), strip(p), mine], h_recv.at[p])
                for u in (2, 3):
                    forward(u, p, 0, right).start()
                    forward(u, p, 1, left).start()

    ffn(0, 0, 1, first=between)

    def near_unit(i, _):
        u = 2 + i
        with jax.named_scope('wait_rows'):
            theirs = pl.ds(pl.multiple_of(2 * (1 - parity) * quarter, 2 * quarter), 2 * quarter)
            here(xr.at[u, :, theirs], f_recv.at[i])
        ffn(1 + i, u, 1)

        @pl.when(i == 0)
        def _():
            with jax.named_scope('near_done'):
                here(xr.at[pl.ds(0, 3)], d_send.at[0])
                pl.semaphore_signal(both, inc=1, device_id={'ep': ep, 'tp': partner}, device_id_type=MESH)
                pl.semaphore_wait(both, 1)
            for copy in far:
                copy.start()

        @pl.when(i == 1)
        def _():
            for h in range(2):
                total(0, 0, 1, h)
                keep_own(0, h)
        return 0

    lax.fori_loop(0, 2, near_unit, 0)
    with jax.named_scope('wait_rows'):
        here(xr.at[pl.ds(4, 2)], d_recv.at[0])
    ffn(3, 4, 2)
    ffn(6, 1, 1, send=False)
    for u in (2, 3):
        for h in range(2):
            total(u - 1, u, 1, h)
            for copy in returns(u, h):
                copy.start()

    rows = tokens // 4
    span = 2 * unit

    def choose(at, j, first_slot, n):
        slot = (lax.broadcasted_iota(jnp.int32, (rows, n), 1) + first_slot).astype(F32)
        return jnp.where(colsT[at, j:j + 1] == slot, 1.0, 0.0).astype(BF16)

    def combine(q, b, n, fresh):
        with jax.named_scope('combine'):
            def block(i, _):
                at = pl.ds(pl.multiple_of(i * rows, rows), rows)
                t = jnp.zeros((rows, 2 * LANES), F32) if fresh else acc[at, :]
                y = jnp.concatenate([ret[h, q, pl.ds(b, n)].reshape(n * span, LANES) for h in range(2)], axis=1)
                for j in range(2):
                    got = jnp.dot(choose(at, j, q * 2 * cap + b * span, n * span), y, preferred_element_type=F32)
                    t = t + colsT[at, 2 + j:3 + j] * got
                acc[at, :] = t
                return 0

            lax.fori_loop(0, 4, block, 0)

    def wait_ret(ref, i):
        with jax.named_scope('wait_ret'):
            here(ref, rt_recv.at[i])

    wait_ret(ret.at[:, 0, 0, other], 5)
    combine(0, 0, 1, True)

    def pick_last(i, _):
        at = pl.ds(pl.multiple_of(i * rows, rows), rows)
        for j in range(2):
            for w, q in enumerate((3, 0)):
                sel[j, at, w * span:(w + 1) * span] = choose(at, j, q * 2 * cap + span, span)
        return 0

    def tail(i, _):
        u = 6 + i
        with jax.named_scope('wait_rows'):
            here(xr.at[u], d_recv.at[1 + i])
        ffn(4 + i, u, 1, also=i == 1)

        @pl.when(i == 0)
        def _():
            lax.fori_loop(0, 4, pick_last, 0)
            for h in range(2):
                total(3, 4, 2, h)
                for w in (4, 5):
                    for copy in returns(w, h):
                        copy.start()
        return 0

    lax.fori_loop(0, 2, tail, 0)

    def combine_near(q):
        wait_ret(ret.at[:, q], q - 1)
        combine(q, 0, 2, False)

    def last_far(h):
        total(5, 7, 1, h)
        for copy in returns(7, h):
            copy.start()

    def last_own(h):
        total(6, 1, 1, h)
        keep_own(1, h)

    for h in range(2):
        total(4, 6, 1, h)
        for copy in returns(6, h):
            copy.start()
    combine_near(1)
    last_far(0)
    combine_near(2)
    last_own(0)
    last_far(1)
    wait_ret(ret.at[:, 3, 0], 2)
    combine(3, 0, 1, False)

    half_rows = tokens // 2

    def place(t, h, p):
        at = slice(None) if p is None else pl.ds(p * half_rows, half_rows)
        return out.at[at, pl.ds(pl.multiple_of((2 * t + h) * LANES, LANES), LANES)]

    def spread(t, h, p, to, i):
        return remote(place(t, h, p), place(t, h, p), ag_send.at[0], ag_recv.at[h, i], ep, to)

    def publish(t, h, p):
        return remote(place(t, h, p), place(t, h, p), p_send.at[0], p_recv.at[0], ep, partner)

    def go(copy):
        copy.start()

    def finish(h):
        wait_ret(ret.at[h, 0, 1, other], 6 + h)
        wait_ret(ret.at[h, 3, 1], 3 + h)
        with jax.named_scope('last'):
            y = jnp.concatenate([ret[h, 3, 1].reshape(span, LANES), ret[h, 0, 1].reshape(span, LANES)], axis=0)
            for i in range(4):
                at = slice(i * rows, (i + 1) * rows)
                t = acc[at, h * LANES:(h + 1) * LANES]
                for j in range(2):
                    got = jnp.dot(sel[j, at, :], y, preferred_element_type=F32)
                    t = t + colsT[at, 2 + j:3 + j] * got
                out[at, pl.ds(pl.multiple_of((2 * tp + h) * LANES, LANES), LANES)] = t.astype(BF16)
                if i == 1:
                    go(spread(tp, h, 0, right, 0))
        go(spread(tp, h, 1, left, 3))
        go(spread(tp, h, 1, right, 1))
        go(spread(tp, h, 0, left, 2))
        go(publish(tp, h, None))

    def relay(h):
        with jax.named_scope('relay'):
            spread(left, h, 0, right, 0).wait_recv()
            go(spread(left, h, 0, right, 4))
            spread(right, h, 1, left, 3).wait_recv()
            go(spread(right, h, 1, left, 5))
            go(publish(left, h, 0))
            go(publish(right, h, 1))

    finish(0)
    last_own(1)
    finish(1)
    relay(0)
    relay(1)
    with jax.named_scope('gather'):
        for h in range(2):
            spread(left, h, 1, right, 1).wait_recv()
            go(publish(left, h, 1))
            spread(right, h, 0, left, 2).wait_recv()
            go(publish(right, h, 0))
        for h in range(2):
            spread(across, h, 0, right, 4).wait_recv()
            go(publish(across, h, 0))
            spread(across, h, 1, left, 5).wait_recv()
            go(publish(across, h, 1))
        here(out.at[:, pl.ds(0, 8 * LANES)], p_recv.at[0])

    with jax.named_scope('drain'):
        here(xs.at[2], d_send.at[1])
        here(w1.at[1], w_send.at[0])
        here(wd.at[1], w_send.at[1])
        here(xr.at[0], f_send.at[0])
        here(rv, rs_send.at[0])
        here(red.at[pl.ds(0, 7)], rt_send.at[0])
        here(out.at[:, pl.ds(0, 6 * LANES)], ag_send.at[0])
        here(out.at[:, pl.ds(0, 8 * LANES)], p_send.at[0])


def solution(mesh):
    n_ep = mesh.shape['ep']
    n_tp = mesh.shape['tp']
    row_spec = P(('dp', 'ep'), None)

    def device_body(x_loc, ids_loc, gates_loc, wg_loc, wu_loc, wd_loc):
        tokens, d_model = x_loc.shape
        n_top = ids_loc.shape[1]
        local_experts, _, ff = wg_loc.shape
        n_experts = local_experts * n_ep
        cap = CAP_NUM * n_top * tokens // (CAP_DEN * n_experts)
        unit = cap // 2
        n_x = n_tp // 2
        n_tile = ff // LANES
        vmem = pltpu.VMEM
        dma = pltpu.SemaphoreType.DMA

        def kernel(*refs):
            moe_kernel(n_ep, n_tp, cap, *refs)

        any_spec = pl.BlockSpec(memory_space=pl.ANY)
        vmem_spec = pl.BlockSpec(memory_space=pltpu.VMEM)
        return pl.pallas_call(
            kernel,
            out_shape=pltpu.VMEM((tokens, d_model), BF16),
            in_specs=[any_spec] * 6,
            out_specs=vmem_spec,
            scratch_shapes=[
                vmem(ids_loc.shape[::-1], jnp.int32),
                vmem(gates_loc.shape[::-1], F32),
                vmem((tokens, d_model), BF16),
                vmem((cap, tokens), BF16),
                vmem((3, 2, unit, d_model), BF16),
                vmem((8, unit, d_model), BF16),
                vmem((2, n_tile, d_model, 2 * LANES), BF16),
                vmem((2, 2, n_x, ff, 2 * LANES), BF16),
                vmem((2, cap, ff), BF16),
                vmem((8, 2, n_x, unit, 2 * LANES), BF16),
                vmem((8, 2, n_x - 1, unit, 2 * LANES), BF16),
                vmem((8, 2, 2, unit, LANES), BF16),
                vmem((2, 4, 2, 2, unit, LANES), BF16),
                vmem((tokens, 2 * LANES), F32),
                vmem((2 * n_experts, tokens), F32),
                vmem((LANES, tokens), F32),
                vmem((tokens, LANES), F32),
                vmem((2, tokens, 4 * unit), BF16),
                dma((3,)), dma((2, 3)), dma((2,)), dma((2,)), dma((3,)),
                dma((1,)), dma((7, 2)), dma((1,)), dma((8,)),
                dma((1,)), dma((2, 6)), dma((1,)), dma((1,)), dma((1,)), dma((2,)), dma((2,)),
                pltpu.SemaphoreType.REGULAR,
            ],
            compiler_params=pltpu.CompilerParams(
                collective_id=0, has_side_effects=True, vmem_limit_bytes=58 * 1024 * 1024),
        )(ids_loc.T, gates_loc.T, x_loc, wg_loc, wu_loc, wd_loc)

    return jax.shard_map(device_body, mesh=mesh,
                         in_specs=(row_spec, row_spec, row_spec, P('ep', None, 'tp'), P('ep', None, 'tp'), P('ep', 'tp', None)),
                         out_specs=row_spec, check_vma=False)
```
